32 devices in a mesh: chan: 4 (over y, x), slab: 8 (over z, core).
Axes of the slice: x: 2, y: 2, z: 4, core: 2. Of those that a mesh axis runs over, the one named last changes fastest.
Arguments:
- taylor_models: float32 [2, 2048, 2048], P(None, 'slab', 'chan'), may hold values from -6 to 6
- gridded_vis: bfloat16 [4, 2, 2048, 2048], P('chan', None, 'slab'), may hold values from -6 to 6
- uv_weight: bfloat16 [4, 2048, 2048], P('chan', 'slab'), may hold values from 0 to 2
- freq_ratio: float32 [4], P('chan'), may hold values from 0.6 to 1.4
- robust_scale: float32 [4], P('chan'), may hold values from 0.25 to 4
Outputs:
- taylor_residual: float32 [2, 2048, 2048], P(None, 'slab', 'chan')
The draws below stay inside these ranges and needn't reach their ends.
All inputs are finite; a program needn't handle non-finite values.
Results may differ from the reference program's by a relative error of at most 0.0003.
Values sent between devices are 32-bit elements; how exact they have to be, the bound alone decides.
A program may use at most 64 MiB of HBM per device.

```python
import math
import jax
import jax.numpy as jnp
from jax import lax

PIX = 2048
TERMS = 2
CHANNELS = 4


def levels(key, dims, cuts, smallest, largest):
    factor_of = 1.0
    for position, parts in cuts:
        steps = jax.random.uniform(jax.random.fold_in(jax.random.fold_in(key, 6), position), (parts,), jnp.float32, smallest / len(cuts), largest / len(cuts))
        factor_of = factor_of * jnp.repeat(jnp.exp(steps), dims[position] // parts).reshape((-1,) + (1,) * (len(dims) - 1 - position))
    return factor_of


def centred(own_key, extent, deviation, bound, pieces=(), dtype=jnp.bfloat16):
    entries = deviation * jax.random.normal(own_key, extent, jnp.float32)
    if pieces:
        entries = entries * levels(own_key, extent, pieces, -0.22, 0.18)
    return jnp.clip(entries, -bound, bound).astype(dtype)


def setup_inputs(seed: int = 0) -> dict:
    keys = jax.random.split(jax.random.key(seed), 6)
    taylor_models = centred(keys[0], (TERMS, PIX, PIX), 1.0, 6.0, ((1, 8), (2, 4)), jnp.float32)
    gridded_vis = centred(keys[1], (CHANNELS, 2, PIX, PIX), 1.0, 6.0, ((0, 4), (2, 8)))
    uv_weight = jnp.clip(2.0 * jax.random.uniform(keys[2], (CHANNELS, PIX, PIX), jnp.float32) ** levels(keys[2], (CHANNELS, PIX, PIX), ((0, 4), (1, 8)), -0.2, 0.2), 0.0, 2.0).astype(jnp.bfloat16)
    freq_ratio = jnp.clip(0.6 + 0.79999995 * jax.random.uniform(keys[3], (CHANNELS,), jnp.float32) ** levels(keys[3], (CHANNELS,), ((0, 4),), -0.2, 0.2), 0.6, 1.4)
    robust_scale = jnp.clip(jnp.exp(math.log(4.0) - 2.7725887 * jax.random.uniform(keys[4], (CHANNELS,), jnp.float32) ** levels(keys[4], (CHANNELS,), ((0, 4),), -0.2, 0.2)), 0.25, 4.0)
    return {"taylor_models": taylor_models, "gridded_vis": gridded_vis, "uv_weight": uv_weight, "freq_ratio": freq_ratio, "robust_scale": robust_scale}


def reference(taylor_models, gridded_vis, uv_weight, freq_ratio, robust_scale):
    def one_channel(carry, item):
        visible, weight, ratio, damping = item
        offset = ratio - 1.0
        sky_image = taylor_models[0]
        for term_index in range(1, TERMS):
            sky_image = sky_image + offset ** term_index * taylor_models[term_index]
        spectrum = jnp.fft.fft2(sky_image, norm="ortho").T
        visible_wide = visible.astype(jnp.float32)
        weight_wide = weight.astype(jnp.float32)
        delta_real = visible_wide[0] - weight_wide * jnp.real(spectrum)
        delta_imag = visible_wide[1] - weight_wide * jnp.imag(spectrum)
        robust = 1.0 / (1.0 + damping * (delta_real * delta_real + delta_imag * delta_imag))
        weighted = lax.complex(robust * delta_real, robust * delta_imag)
        residual = jnp.real(jnp.fft.ifft2(weighted.T, norm="ortho"))
        layers = [residual]
        for term_index in range(1, TERMS):
            layers.append(offset ** term_index * residual)
        return carry + jnp.stack(layers), None

    initial = jnp.zeros((TERMS, PIX, PIX), jnp.float32)
    total, _ = lax.scan(one_channel, initial, (gridded_vis, uv_weight, freq_ratio, robust_scale))
    return total
```

```python
import math

import jax
import jax.numpy as jnp
from jax import lax
from jax.sharding import PartitionSpec as P

PIX = 2048
TERMS = 2


HIGHEST = lax.Precision.HIGH


def dft_table(points, direction):
    steps_all = jnp.arange(points, dtype=jnp.int32)
    product = steps_all[:, None] * steps_all[None, :] % points
    angles = product.astype(jnp.float32) * (2.0 * math.pi / points)
    return (jnp.cos(angles), direction * jnp.sin(angles))


def twiddle_table(outer_points, inner_points, direction):
    outer_steps = jnp.arange(outer_points, dtype=jnp.int32)
    inner_steps = jnp.arange(inner_points, dtype=jnp.int32)
    overall = outer_points * inner_points
    product = outer_steps[:, None] * inner_steps[None, :] % overall
    angles = product.astype(jnp.float32) * (2.0 * math.pi / overall)
    return (jnp.cos(angles), direction * jnp.sin(angles))


def complex_product(formula, left_real, left_imag, table_real, table_imag):
    out_real = jnp.einsum(formula, left_real, table_real, precision=HIGHEST) - jnp.einsum(
        formula, left_imag, table_imag, precision=HIGHEST
    )
    out_imag = jnp.einsum(formula, left_real, table_imag, precision=HIGHEST) + jnp.einsum(
        formula, left_imag, table_real, precision=HIGHEST
    )
    return (out_real, out_imag)


def rotate(left_real, left_imag, table_real, table_imag):
    return (
        left_real * table_real - left_imag * table_imag,
        left_real * table_imag + left_imag * table_real,
    )


def local(taylor_models, gridded_vis, uv_weight, freq_ratio, robust_scale):
    inner_count = 128
    outer_count = PIX // inner_count
    chans = lax.axis_size("chan")
    slabs = lax.axis_size("slab")
    rows = taylor_models.shape[1]
    cols = taylor_models.shape[2]
    sub = rows // chans
    col_count = PIX // slabs
    outer_cos, outer_sin = dft_table(outer_count, -1.0)
    inner_cos, inner_sin = dft_table(inner_count, -1.0)
    twist_cos, twist_sin = twiddle_table(outer_count, inner_count, -1.0)
    offsets = lax.all_gather(freq_ratio, "chan", axis=0, tiled=True) - 1.0

    pieces = taylor_models.reshape(TERMS, chans, sub, cols).transpose(1, 0, 2, 3)
    pieces = lax.all_to_all(pieces, "chan", split_axis=0, concat_axis=0, tiled=True)
    layered = pieces.transpose(1, 2, 0, 3).reshape(TERMS * sub, outer_count, inner_count)
    part_real = jnp.einsum("yba,jb->yja", layered, outer_cos, precision=HIGHEST)
    part_imag = jnp.einsum("yba,jb->yja", layered, outer_sin, precision=HIGHEST)
    turned_real, turned_imag = rotate(part_real, part_imag, twist_cos, twist_sin)
    spec_real, spec_imag = complex_product(
        "yja,ka->kjy", turned_real, turned_imag, inner_cos, inner_sin
    )
    outgoing = jnp.stack(
        [
            spec_real.reshape(slabs, col_count, TERMS * sub),
            spec_imag.reshape(slabs, col_count, TERMS * sub),
        ],
        axis=1,
    )
    arrived = lax.all_to_all(outgoing, "slab", split_axis=0, concat_axis=0, tiled=True)
    arrived = arrived.reshape(slabs, 2, col_count, TERMS, sub)
    arrived = arrived.transpose(3, 1, 2, 0, 4).reshape(TERMS, 2, col_count, slabs * sub)
    mixed = arrived[0][None] + offsets[:, None, None, None] * arrived[1][None]
    mixed = lax.all_to_all(mixed, "chan", split_axis=0, concat_axis=0, tiled=True)
    columns = mixed.reshape(chans, 2, col_count, slabs, sub).transpose(1, 2, 3, 0, 4)
    layered_cols = columns.reshape(2, col_count, outer_count, inner_count)
    part_real, part_imag = complex_product(
        "uba,jb->uja", layered_cols[0], layered_cols[1], outer_cos, outer_sin
    )
    turned_real, turned_imag = rotate(part_real, part_imag, twist_cos, twist_sin)
    freq_real, freq_imag = complex_product(
        "uja,ka->ujk", turned_real, turned_imag, inner_cos, inner_sin
    )
    freq_real = freq_real / PIX
    freq_imag = freq_imag / PIX
    weight = (
        uv_weight[0]
        .astype(jnp.float32)
        .reshape(col_count, inner_count, outer_count)
        .transpose(0, 2, 1)
    )
    visible = (
        gridded_vis[0]
        .astype(jnp.float32)
        .reshape(2, col_count, inner_count, outer_count)
        .transpose(0, 1, 3, 2)
    )
    delta_real = visible[0] - weight * freq_real
    delta_imag = visible[1] - weight * freq_imag
    robust = 1.0 / (1.0 + robust_scale[0] * (delta_real * delta_real + delta_imag * delta_imag))
    weighted_real = robust * delta_real
    weighted_imag = robust * delta_imag
    back_real, back_imag = complex_product(
        "ujk,ak->uja", weighted_real, weighted_imag, inner_cos, -inner_sin
    )
    back_real, back_imag = rotate(back_real, back_imag, twist_cos, -twist_sin)
    back_real, back_imag = complex_product(
        "uja,bj->uba", back_real, back_imag, outer_cos, -outer_sin
    )
    back = jnp.stack([back_real, back_imag]).reshape(2, col_count, slabs, chans, sub)
    back = back.transpose(3, 0, 1, 2, 4).reshape(chans, 2, col_count, slabs * sub)
    back = lax.all_to_all(back, "chan", split_axis=0, concat_axis=0, tiled=True)
    total = jnp.stack(
        [jnp.sum(back * offsets[:, None, None, None] ** t, axis=0) for t in range(TERMS)]
    )
    total = total.reshape(TERMS, 2, col_count, slabs, sub).transpose(3, 1, 2, 0, 4)
    total = total.reshape(slabs, 2, col_count, TERMS * sub)
    total = lax.all_to_all(total, "slab", split_axis=0, concat_axis=0, tiled=True)
    layered_rows = total.transpose(1, 0, 2, 3).reshape(2, inner_count, outer_count, TERMS * sub)
    last_real, last_imag = complex_product(
        "kjy,ak->ajy", layered_rows[0], layered_rows[1], inner_cos, -inner_sin
    )
    last_real, last_imag = rotate(
        last_real, last_imag, twist_cos.T[:, :, None], -twist_sin.T[:, :, None]
    )
    image_out = jnp.einsum("ajy,bj->yba", last_real, outer_cos, precision=HIGHEST) + jnp.einsum(
        "ajy,bj->yba", last_imag, outer_sin, precision=HIGHEST
    )
    image_out = image_out.reshape(TERMS, sub, chans, cols).transpose(2, 0, 1, 3) / PIX
    tiles = lax.all_to_all(image_out, "chan", split_axis=0, concat_axis=0, tiled=True)
    return tiles.transpose(1, 0, 2, 3).reshape(TERMS, rows, cols)


def solution(mesh):
    placed = (
        P(None, "slab", "chan"),
        P("chan", None, "slab", None),
        P("chan", "slab", None),
        P("chan"),
        P("chan"),
    )
    return jax.shard_map(
        local, mesh=mesh, in_specs=placed, out_specs=P(None, "slab", "chan"), check_vma=False
    )
```

```python
import functools
import math

import jax
import jax.numpy as jnp
import numpy as np
from jax import lax
from jax.experimental import pallas as pl
from jax.experimental.pallas import tpu as pltpu
from jax.sharding import PartitionSpec as P

PIX = 2048
TERMS = 2


HIGHEST = lax.Precision.HIGH


def dft_table(points, direction):
    steps_all = jnp.arange(points, dtype=jnp.int32)
    product = steps_all[:, None] * steps_all[None, :] % points
    angles = product.astype(jnp.float32) * (2.0 * math.pi / points)
    return (jnp.cos(angles), direction * jnp.sin(angles))


def twiddle_table(outer_points, inner_points, direction):
    outer_steps = jnp.arange(outer_points, dtype=jnp.int32)
    inner_steps = jnp.arange(inner_points, dtype=jnp.int32)
    overall = outer_points * inner_points
    product = outer_steps[:, None] * inner_steps[None, :] % overall
    angles = product.astype(jnp.float32) * (2.0 * math.pi / overall)
    return (jnp.cos(angles), direction * jnp.sin(angles))


def complex_product(formula, left_real, left_imag, table_real, table_imag):
    out_real = jnp.einsum(formula, left_real, table_real, precision=HIGHEST) - jnp.einsum(
        formula, left_imag, table_imag, precision=HIGHEST
    )
    out_imag = jnp.einsum(formula, left_real, table_imag, precision=HIGHEST) + jnp.einsum(
        formula, left_imag, table_real, precision=HIGHEST
    )
    return (out_real, out_imag)


def rotate(left_real, left_imag, table_real, table_imag):
    return (
        left_real * table_real - left_imag * table_imag,
        left_real * table_imag + left_imag * table_real,
    )


def local_general(taylor_models, gridded_vis, uv_weight, freq_ratio, robust_scale):
    inner_count = 128
    outer_count = PIX // inner_count
    chans = lax.axis_size("chan")
    slabs = lax.axis_size("slab")
    rows = taylor_models.shape[1]
    cols = taylor_models.shape[2]
    sub = rows // chans
    col_count = PIX // slabs
    outer_cos, outer_sin = dft_table(outer_count, -1.0)
    inner_cos, inner_sin = dft_table(inner_count, -1.0)
    twist_cos, twist_sin = twiddle_table(outer_count, inner_count, -1.0)
    offsets = lax.all_gather(freq_ratio, "chan", axis=0, tiled=True) - 1.0

    pieces = taylor_models.reshape(TERMS, chans, sub, cols).transpose(1, 0, 2, 3)
    pieces = lax.all_to_all(pieces, "chan", split_axis=0, concat_axis=0, tiled=True)
    layered = pieces.transpose(1, 2, 0, 3).reshape(TERMS * sub, outer_count, inner_count)
    part_real = jnp.einsum("yba,jb->yja", layered, outer_cos, precision=HIGHEST)
    part_imag = jnp.einsum("yba,jb->yja", layered, outer_sin, precision=HIGHEST)
    turned_real, turned_imag = rotate(part_real, part_imag, twist_cos, twist_sin)
    spec_real, spec_imag = complex_product(
        "yja,ka->kjy", turned_real, turned_imag, inner_cos, inner_sin
    )
    outgoing = jnp.stack(
        [
            spec_real.reshape(slabs, col_count, TERMS * sub),
            spec_imag.reshape(slabs, col_count, TERMS * sub),
        ],
        axis=1,
    )
    arrived = lax.all_to_all(outgoing, "slab", split_axis=0, concat_axis=0, tiled=True)
    arrived = arrived.reshape(slabs, 2, col_count, TERMS, sub)
    arrived = arrived.transpose(3, 1, 2, 0, 4).reshape(TERMS, 2, col_count, slabs * sub)
    mixed = arrived[0][None] + offsets[:, None, None, None] * arrived[1][None]
    mixed = lax.all_to_all(mixed, "chan", split_axis=0, concat_axis=0, tiled=True)
    columns = mixed.reshape(chans, 2, col_count, slabs, sub).transpose(1, 2, 3, 0, 4)
    layered_cols = columns.reshape(2, col_count, outer_count, inner_count)
    part_real, part_imag = complex_product(
        "uba,jb->uja", layered_cols[0], layered_cols[1], outer_cos, outer_sin
    )
    turned_real, turned_imag = rotate(part_real, part_imag, twist_cos, twist_sin)
    freq_real, freq_imag = complex_product(
        "uja,ka->ujk", turned_real, turned_imag, inner_cos, inner_sin
    )
    freq_real = freq_real / PIX
    freq_imag = freq_imag / PIX
    weight = (
        uv_weight[0]
        .astype(jnp.float32)
        .reshape(col_count, inner_count, outer_count)
        .transpose(0, 2, 1)
    )
    visible = (
        gridded_vis[0]
        .astype(jnp.float32)
        .reshape(2, col_count, inner_count, outer_count)
        .transpose(0, 1, 3, 2)
    )
    delta_real = visible[0] - weight * freq_real
    delta_imag = visible[1] - weight * freq_imag
    robust = 1.0 / (1.0 + robust_scale[0] * (delta_real * delta_real + delta_imag * delta_imag))
    weighted_real = robust * delta_real
    weighted_imag = robust * delta_imag
    back_real, back_imag = complex_product(
        "ujk,ak->uja", weighted_real, weighted_imag, inner_cos, -inner_sin
    )
    back_real, back_imag = rotate(back_real, back_imag, twist_cos, -twist_sin)
    back_real, back_imag = complex_product(
        "uja,bj->uba", back_real, back_imag, outer_cos, -outer_sin
    )
    back = jnp.stack([back_real, back_imag]).reshape(2, col_count, slabs, chans, sub)
    back = back.transpose(3, 0, 1, 2, 4).reshape(chans, 2, col_count, slabs * sub)
    back = lax.all_to_all(back, "chan", split_axis=0, concat_axis=0, tiled=True)
    total = jnp.stack(
        [jnp.sum(back * offsets[:, None, None, None] ** t, axis=0) for t in range(TERMS)]
    )
    total = total.reshape(TERMS, 2, col_count, slabs, sub).transpose(3, 1, 2, 0, 4)
    total = total.reshape(slabs, 2, col_count, TERMS * sub)
    total = lax.all_to_all(total, "slab", split_axis=0, concat_axis=0, tiled=True)
    layered_rows = total.transpose(1, 0, 2, 3).reshape(2, inner_count, outer_count, TERMS * sub)
    last_real, last_imag = complex_product(
        "kjy,ak->ajy", layered_rows[0], layered_rows[1], inner_cos, -inner_sin
    )
    last_real, last_imag = rotate(
        last_real, last_imag, twist_cos.T[:, :, None], -twist_sin.T[:, :, None]
    )
    image_out = jnp.einsum("ajy,bj->yba", last_real, outer_cos, precision=HIGHEST) + jnp.einsum(
        "ajy,bj->yba", last_imag, outer_sin, precision=HIGHEST
    )
    image_out = image_out.reshape(TERMS, sub, chans, cols).transpose(2, 0, 1, 3) / PIX
    tiles = lax.all_to_all(image_out, "chan", split_axis=0, concat_axis=0, tiled=True)
    return tiles.transpose(1, 0, 2, 3).reshape(TERMS, rows, cols)


CHUNKS = 4
GROUP = 8
MESH = pl.DeviceIdType.MESH


def lane_tables(slabs, chans, sub):
    j = np.arange(chans)[:, None, None, None]
    v0 = np.arange(slabs)[None, :, None, None]
    r = np.arange(sub)[None, None, :, None]
    k = np.arange(sub)[None, None, None, :]
    phase = ((chans * r + j) * (v0 + slabs * k)) % PIX
    cos = np.cos(2.0 * np.pi * phase / PIX) / PIX
    sin = -np.sin(2.0 * np.pi * phase / PIX) / PIX
    top = np.concatenate([cos, sin], axis=3)
    low = np.concatenate([-sin, cos], axis=3)
    table = np.concatenate([top, low], axis=2).reshape(chans * slabs, 2 * sub, 2 * sub)
    table = table.astype(np.float32)
    high = table.astype(jnp.bfloat16)
    return high, (table - high.astype(np.float32)).astype(jnp.bfloat16)


def sort_table(slabs, sub):
    span = slabs * sub
    source = jnp.arange(2 * span, dtype=jnp.int32)
    part, v = source // span, source % span
    target = (v % slabs) * (2 * sub) + part * sub + v // slabs
    return (target[:, None] == jnp.arange(2 * span, dtype=jnp.int32)[None, :]).astype(jnp.bfloat16)


def middle_kernel(
    slabs, chans, g_ref, vis_ref, wt_ref, off_ref, rs_ref, high_ref, low_ref, sort_ref, q_ref,
    zin, mix, spec, back, landed, qsend, offs, work, vsort, wsort,
    z_send, z_recv, c_send, c_recv, b_send, b_recv, q_send, q_recv, o_send, o_recv,
):
    slab = lax.axis_index("slab")
    chan = lax.axis_index("chan")
    unit = g_ref.shape[3]
    lanes = g_ref.shape[4]
    half = lanes // 2
    span = slabs * half

    def slab_peer(d):
        return lax.rem(slab + d, slabs)

    def slab_from(d):
        return lax.rem(slab + slabs - d, slabs)

    def chan_peer(d):
        return lax.rem(chan + d, chans)

    def chan_from(d):
        return lax.rem(chan + chans - d, chans)

    def z_copy(c, d, owner):
        return pltpu.make_async_remote_copy(
            src_ref=g_ref.at[c, slab_peer(d)], dst_ref=zin.at[c, owner],
            send_sem=z_send.at[c, d], recv_sem=z_recv.at[c, d],
            device_id=(chan, slab_peer(d)), device_id_type=MESH)

    def c_copy(c, d, owner):
        return pltpu.make_async_remote_copy(
            src_ref=mix.at[c, d - 1], dst_ref=spec.at[c, owner],
            send_sem=c_send.at[c, d], recv_sem=c_recv.at[c, d],
            device_id=(chan_peer(d), slab), device_id_type=MESH)

    def b_copy(c, d, owner):
        return pltpu.make_async_remote_copy(
            src_ref=back.at[c, d - 1], dst_ref=landed.at[c, owner],
            send_sem=b_send.at[c, d], recv_sem=b_recv.at[c, d],
            device_id=(chan_peer(d), slab), device_id_type=MESH)

    def q_copy(c, d, owner):
        return pltpu.make_async_remote_copy(
            src_ref=qsend.at[c, slab_peer(d)], dst_ref=q_ref.at[c, owner],
            send_sem=q_send.at[c, d], recv_sem=q_recv.at[c, d],
            device_id=(chan, slab_peer(d)), device_id_type=MESH)

    def o_copy(d, owner):
        return pltpu.make_async_remote_copy(
            src_ref=off_ref, dst_ref=offs.at[owner],
            send_sem=o_send.at[d], recv_sem=o_recv.at[d],
            device_id=(chan_peer(d), slab), device_id_type=MESH)

    barrier = pltpu.get_barrier_semaphore()
    for d in range(1, slabs):
        pl.semaphore_signal(barrier, inc=1, device_id=(chan, slab_peer(d)), device_id_type=MESH)
    for d in range(1, chans):
        pl.semaphore_signal(barrier, inc=1, device_id=(chan_peer(d), slab), device_id_type=MESH)
    pl.semaphore_wait(barrier, slabs + chans - 2)

    for d in range(1, chans):
        o_copy(d, chan).start()

    @pl.loop(0, CHUNKS)
    def _(c):
        for d in range(1, slabs):
            z_copy(c, d, slab).start()

    offs[chan] = off_ref[...]

    @pl.loop(0, CHUNKS)
    def _(c):
        zin[c, slab] = g_ref[c, slab]
        rows = pl.ds(pl.multiple_of(c * unit, unit), unit)
        for jj in range(chans):
            at = pl.ds(jj * span, span)
            pair = jnp.concatenate([vis_ref[0, rows, at], vis_ref[1, rows, at]], axis=1)
            vsort[c, jj] = jnp.dot(pair, sort_ref[...], preferred_element_type=jnp.float32)
            pair = jnp.concatenate([wt_ref[rows, at], wt_ref[rows, at]], axis=1)
            wsort[c, jj] = jnp.dot(pair, sort_ref[...], preferred_element_type=jnp.float32)

    for d in range(1, chans):
        o_copy(d, chan_from(d)).wait_recv()

    lane = lax.broadcasted_iota(jnp.int32, (GROUP, lanes), 1)
    sign = jnp.where(lane < half, -1.0, 1.0)

    def times_i(x, direction):
        return pltpu.roll(x, half, 1) * (sign * direction)

    def four(x0, x1, x2, x3, direction):
        s0, s1, t0, t1 = x0 + x2, x0 - x2, x1 + x3, times_i(x1 - x3, direction)
        return s0 + t0, s1 + t1, s0 - t0, s1 - t1

    def eight(x, direction):
        root = math.sqrt(0.5)
        even = four(x[0], x[2], x[4], x[6], direction)
        odd = four(x[1], x[3], x[5], x[7], direction)
        odd = (
            odd[0],
            (odd[1] + times_i(odd[1], direction)) * root,
            times_i(odd[2], direction),
            (times_i(odd[3], direction) - odd[3]) * root,
        )
        return [e + o for e, o in zip(even, odd)] + [e - o for e, o in zip(even, odd)]

    def split(x):
        high = x.astype(jnp.bfloat16)
        return high, (x - high.astype(jnp.float32)).astype(jnp.bfloat16)

    def product(x, t, dims):
        high, low = split(x)
        dot = functools.partial(
            lax.dot_general, dimension_numbers=(dims, ((), ())),
            preferred_element_type=jnp.float32)
        wide = dot(high, high_ref[t])
        return wide + (dot(low, high_ref[t]) + dot(high, low_ref[t]))

    def spread(c):
        for d in range(1, slabs):
            z_copy(c, d, slab_from(d)).wait_recv()

        @pl.loop(0, slabs)
        def _(s):
            base, slope = zin[c, s, 0], zin[c, s, 1]
            spec[c, chan, s] = base + offs[chan][0:1, :] * slope
            for d in range(1, chans):
                mix[c, d - 1, s] = base + offs[chan_peer(d)][0:1, :] * slope

        for d in range(1, chans):
            c_copy(c, d, chan).start()

    def weigh(c):
        for d in range(1, chans):
            c_copy(c, d, chan_from(d)).wait_recv()
        damping = rs_ref[0:1, :]

        @pl.loop(0, unit // GROUP)
        def _(i):
            rows = pl.ds(pl.multiple_of(i * GROUP, GROUP), GROUP)
            for j in range(chans):
                out = eight([spec[c, j, s, rows, :] for s in range(slabs)], -1.0)
                for v0 in range(slabs):
                    work[j * slabs + v0, rows, :] = out[v0]

        @pl.loop(0, chans * slabs)
        def _(t):
            work[t] = product(work[t], t, ((1,), (0,)))

        @pl.loop(0, unit // GROUP)
        def _(i):
            rows = pl.ds(pl.multiple_of(i * GROUP, GROUP), GROUP)
            for v0 in range(slabs):
                at = pl.ds(v0 * lanes, lanes)
                found = four(*[work[j * slabs + v0, rows, :] for j in range(chans)], -1.0)
                kept = []
                for jj in range(chans):
                    delta = vsort[c, jj, rows, at] - wsort[c, jj, rows, at] * found[jj]
                    power = delta * delta
                    power = power + pltpu.roll(power, half, 1)
                    kept.append(delta / (1.0 + damping * power))
                out = four(*kept, 1.0)
                for j in range(chans):
                    work[j * slabs + v0, rows, :] = out[j]

        @pl.loop(0, chans * slabs)
        def _(t):
            work[t] = product(work[t], t, ((1,), (1,)))

        @pl.loop(0, unit // GROUP)
        def _(i):
            rows = pl.ds(pl.multiple_of(i * GROUP, GROUP), GROUP)
            for d in range(chans):
                first = chan_peer(d) * slabs
                out = eight([work[first + v0, rows, :] for v0 in range(slabs)], 1.0)
                for s in range(slabs):
                    if d == 0:
                        landed[c, chan, s, rows, :] = out[s]
                    else:
                        back[c, d - 1, s, rows, :] = out[s]

        for d in range(1, chans):
            b_copy(c, d, chan).start()

    def gather(c):
        for d in range(1, chans):
            b_copy(c, d, chan_from(d)).wait_recv()

        @pl.loop(0, slabs)
        def _(s):
            parts = [landed[c, j, s] for j in range(chans)]
            qsend[c, s, 0] = (parts[0] + parts[1]) + (parts[2] + parts[3])
            scaled = [parts[j] * offs[j][0:1, :] for j in range(chans)]
            qsend[c, s, 1] = (scaled[0] + scaled[1]) + (scaled[2] + scaled[3])

        q_ref[c, slab] = qsend[c, slab]
        for d in range(1, slabs):
            q_copy(c, d, slab).start()

    @pl.loop(0, CHUNKS + 3)
    def _(step):
        @pl.when(step < CHUNKS)
        def _():
            spread(step)

        @pl.when(jnp.logical_and(step >= 1, step < CHUNKS + 1))
        def _():
            weigh(step - 1)

        @pl.when(step >= 3)
        def _():
            gather(step - 3)

    @pl.loop(0, CHUNKS)
    def _(c):
        for d in range(1, slabs):
            q_copy(c, d, slab_from(d)).wait_recv()
            q_copy(c, d, slab).wait_send()
            z_copy(c, d, slab).wait_send()
        for d in range(1, chans):
            c_copy(c, d, chan).wait_send()
            b_copy(c, d, chan).wait_send()

    for d in range(1, chans):
        o_copy(d, chan).wait_send()


def middle(g, vis, weight, offset, damping, slabs, chans):
    unit, lanes = g.shape[3], g.shape[4]
    sub = lanes // 2
    high, low = lane_tables(slabs, chans, sub)
    vmem = pl.BlockSpec(memory_space=pltpu.VMEM)
    f32 = jnp.float32
    tile = (unit, lanes)
    return pl.pallas_call(
        functools.partial(middle_kernel, slabs, chans),
        out_shape=jax.ShapeDtypeStruct((CHUNKS, slabs, TERMS) + tile, f32),
        in_specs=[vmem] * 8,
        out_specs=vmem,
        scratch_shapes=[
            pltpu.VMEM((CHUNKS, slabs, TERMS) + tile, f32),
            pltpu.VMEM((CHUNKS, chans - 1, slabs) + tile, f32),
            pltpu.VMEM((CHUNKS, chans, slabs) + tile, f32),
            pltpu.VMEM((CHUNKS, chans - 1, slabs) + tile, f32),
            pltpu.VMEM((CHUNKS, chans, slabs) + tile, f32),
            pltpu.VMEM((CHUNKS, slabs, TERMS) + tile, f32),
            pltpu.VMEM((chans, 8, lanes), f32),
            pltpu.VMEM((chans * slabs,) + tile, f32),
            pltpu.VMEM((CHUNKS, chans, unit, slabs * lanes), f32),
            pltpu.VMEM((CHUNKS, chans, unit, slabs * lanes), f32),
        ]
        + [pltpu.SemaphoreType.DMA((CHUNKS, slabs))] * 2
        + [pltpu.SemaphoreType.DMA((CHUNKS, chans))] * 4
        + [pltpu.SemaphoreType.DMA((CHUNKS, slabs))] * 2
        + [pltpu.SemaphoreType.DMA((chans,))] * 2,
        compiler_params=pltpu.CompilerParams(
            collective_id=0, has_side_effects=True, vmem_limit_bytes=60 * 1024 * 1024
        ),
    )(
        g, vis, weight,
        jnp.broadcast_to(offset, (8, lanes)), jnp.broadcast_to(damping, (8, lanes)),
        jnp.asarray(high), jnp.asarray(low), sort_table(slabs, sub),
    )


def local(taylor_models, gridded_vis, uv_weight, freq_ratio, robust_scale):
    chans = lax.axis_size("chan")
    slabs = lax.axis_size("slab")
    rows = taylor_models.shape[1]
    cols = taylor_models.shape[2]
    sub = rows // chans
    if slabs != 8 or chans != 4 or 2 * sub != 128:
        return local_general(taylor_models, gridded_vis, uv_weight, freq_ratio, robust_scale)
    inner_count = 128
    outer_count = PIX // inner_count
    col_count = PIX // slabs
    unit = col_count // CHUNKS
    outer_cos, outer_sin = dft_table(outer_count, -1.0)
    inner_cos, inner_sin = dft_table(inner_count, -1.0)
    twist_cos, twist_sin = twiddle_table(outer_count, inner_count, -1.0)

    pieces = taylor_models.reshape(TERMS, sub, chans, cols).transpose(2, 0, 1, 3)
    pieces = lax.all_to_all(pieces, "chan", split_axis=0, concat_axis=0, tiled=True)
    layered = pieces.transpose(1, 2, 0, 3).reshape(TERMS * sub, outer_count, inner_count)
    part_real = jnp.einsum("yba,jb->yja", layered, outer_cos, precision=HIGHEST)
    part_imag = jnp.einsum("yba,jb->yja", layered, outer_sin, precision=HIGHEST)
    turned_real, turned_imag = rotate(part_real, part_imag, twist_cos, twist_sin)
    spec_real, spec_imag = complex_product(
        "yja,ka->kjy", turned_real, turned_imag, inner_cos, inner_sin
    )
    outgoing = jnp.stack([spec_real, spec_imag], axis=2)
    outgoing = outgoing.reshape(slabs, CHUNKS, unit, 2, TERMS, sub).transpose(1, 0, 4, 2, 3, 5)
    outgoing = outgoing.reshape(CHUNKS, slabs, TERMS, unit, 2 * sub)
    total = middle(
        outgoing, gridded_vis[0], uv_weight[0], freq_ratio[0] - 1.0, robust_scale[0], slabs, chans
    )
    total = total.reshape(CHUNKS, slabs, TERMS, unit, 2, sub).transpose(4, 1, 0, 3, 2, 5)
    layered_rows = total.reshape(2, inner_count, outer_count, TERMS * sub)
    last_real, last_imag = complex_product(
        "kjy,ak->ajy", layered_rows[0], layered_rows[1], inner_cos, -inner_sin
    )
    last_real, last_imag = rotate(
        last_real, last_imag, twist_cos.T[:, :, None], -twist_sin.T[:, :, None]
    )
    image_out = jnp.einsum("ajy,bj->yba", last_real, outer_cos, precision=HIGHEST) + jnp.einsum(
        "ajy,bj->yba", last_imag, outer_sin, precision=HIGHEST
    )
    image_out = image_out.reshape(TERMS, sub, chans, cols).transpose(2, 0, 1, 3)
    tiles = lax.all_to_all(image_out, "chan", split_axis=0, concat_axis=0, tiled=True)
    return tiles.transpose(1, 2, 0, 3).reshape(TERMS, rows, cols)


def solution(mesh):
    placed = (
        P(None, "slab", "chan"),
        P("chan", None, "slab", None),
        P("chan", "slab", None),
        P("chan"),
        P("chan"),
    )
    return jax.shard_map(
        local, mesh=mesh, in_specs=placed, out_specs=P(None, "slab", "chan"), check_vma=False
    )
```

```python
import functools
import math

import jax
import jax.numpy as jnp
import numpy as np
from jax import lax
from jax.experimental import pallas as pl
from jax.experimental.pallas import tpu as pltpu
from jax.sharding import PartitionSpec as P

PIX = 2048
TERMS = 2


HIGHEST = lax.Precision.HIGH


def dft_table(points, direction):
    steps_all = jnp.arange(points, dtype=jnp.int32)
    product = steps_all[:, None] * steps_all[None, :] % points
    angles = product.astype(jnp.float32) * (2.0 * math.pi / points)
    return (jnp.cos(angles), direction * jnp.sin(angles))


def twiddle_table(outer_points, inner_points, direction):
    outer_steps = jnp.arange(outer_points, dtype=jnp.int32)
    inner_steps = jnp.arange(inner_points, dtype=jnp.int32)
    overall = outer_points * inner_points
    product = outer_steps[:, None] * inner_steps[None, :] % overall
    angles = product.astype(jnp.float32) * (2.0 * math.pi / overall)
    return (jnp.cos(angles), direction * jnp.sin(angles))


def complex_product(formula, left_real, left_imag, table_real, table_imag):
    out_real = jnp.einsum(formula, left_real, table_real, precision=HIGHEST) - jnp.einsum(
        formula, left_imag, table_imag, precision=HIGHEST
    )
    out_imag = jnp.einsum(formula, left_real, table_imag, precision=HIGHEST) + jnp.einsum(
        formula, left_imag, table_real, precision=HIGHEST
    )
    return (out_real, out_imag)


def rotate(left_real, left_imag, table_real, table_imag):
    return (
        left_real * table_real - left_imag * table_imag,
        left_real * table_imag + left_imag * table_real,
    )


def local_general(taylor_models, gridded_vis, uv_weight, freq_ratio, robust_scale):
    inner_count = 128
    outer_count = PIX // inner_count
    chans = lax.axis_size("chan")
    slabs = lax.axis_size("slab")
    rows = taylor_models.shape[1]
    cols = taylor_models.shape[2]
    sub = rows // chans
    col_count = PIX // slabs
    outer_cos, outer_sin = dft_table(outer_count, -1.0)
    inner_cos, inner_sin = dft_table(inner_count, -1.0)
    twist_cos, twist_sin = twiddle_table(outer_count, inner_count, -1.0)
    offsets = lax.all_gather(freq_ratio, "chan", axis=0, tiled=True) - 1.0

    pieces = taylor_models.reshape(TERMS, chans, sub, cols).transpose(1, 0, 2, 3)
    pieces = lax.all_to_all(pieces, "chan", split_axis=0, concat_axis=0, tiled=True)
    layered = pieces.transpose(1, 2, 0, 3).reshape(TERMS * sub, outer_count, inner_count)
    part_real = jnp.einsum("yba,jb->yja", layered, outer_cos, precision=HIGHEST)
    part_imag = jnp.einsum("yba,jb->yja", layered, outer_sin, precision=HIGHEST)
    turned_real, turned_imag = rotate(part_real, part_imag, twist_cos, twist_sin)
    spec_real, spec_imag = complex_product(
        "yja,ka->kjy", turned_real, turned_imag, inner_cos, inner_sin
    )
    outgoing = jnp.stack(
        [
            spec_real.reshape(slabs, col_count, TERMS * sub),
            spec_imag.reshape(slabs, col_count, TERMS * sub),
        ],
        axis=1,
    )
    arrived = lax.all_to_all(outgoing, "slab", split_axis=0, concat_axis=0, tiled=True)
    arrived = arrived.reshape(slabs, 2, col_count, TERMS, sub)
    arrived = arrived.transpose(3, 1, 2, 0, 4).reshape(TERMS, 2, col_count, slabs * sub)
    mixed = arrived[0][None] + offsets[:, None, None, None] * arrived[1][None]
    mixed = lax.all_to_all(mixed, "chan", split_axis=0, concat_axis=0, tiled=True)
    columns = mixed.reshape(chans, 2, col_count, slabs, sub).transpose(1, 2, 3, 0, 4)
    layered_cols = columns.reshape(2, col_count, outer_count, inner_count)
    part_real, part_imag = complex_product(
        "uba,jb->uja", layered_cols[0], layered_cols[1], outer_cos, outer_sin
    )
    turned_real, turned_imag = rotate(part_real, part_imag, twist_cos, twist_sin)
    freq_real, freq_imag = complex_product(
        "uja,ka->ujk", turned_real, turned_imag, inner_cos, inner_sin
    )
    freq_real = freq_real / PIX
    freq_imag = freq_imag / PIX
    weight = (
        uv_weight[0]
        .astype(jnp.float32)
        .reshape(col_count, inner_count, outer_count)
        .transpose(0, 2, 1)
    )
    visible = (
        gridded_vis[0]
        .astype(jnp.float32)
        .reshape(2, col_count, inner_count, outer_count)
        .transpose(0, 1, 3, 2)
    )
    delta_real = visible[0] - weight * freq_real
    delta_imag = visible[1] - weight * freq_imag
    robust = 1.0 / (1.0 + robust_scale[0] * (delta_real * delta_real + delta_imag * delta_imag))
    weighted_real = robust * delta_real
    weighted_imag = robust * delta_imag
    back_real, back_imag = complex_product(
        "ujk,ak->uja", weighted_real, weighted_imag, inner_cos, -inner_sin
    )
    back_real, back_imag = rotate(back_real, back_imag, twist_cos, -twist_sin)
    back_real, back_imag = complex_product(
        "uja,bj->uba", back_real, back_imag, outer_cos, -outer_sin
    )
    back = jnp.stack([back_real, back_imag]).reshape(2, col_count, slabs, chans, sub)
    back = back.transpose(3, 0, 1, 2, 4).reshape(chans, 2, col_count, slabs * sub)
    back = lax.all_to_all(back, "chan", split_axis=0, concat_axis=0, tiled=True)
    total = jnp.stack(
        [jnp.sum(back * offsets[:, None, None, None] ** t, axis=0) for t in range(TERMS)]
    )
    total = total.reshape(TERMS, 2, col_count, slabs, sub).transpose(3, 1, 2, 0, 4)
    total = total.reshape(slabs, 2, col_count, TERMS * sub)
    total = lax.all_to_all(total, "slab", split_axis=0, concat_axis=0, tiled=True)
    layered_rows = total.transpose(1, 0, 2, 3).reshape(2, inner_count, outer_count, TERMS * sub)
    last_real, last_imag = complex_product(
        "kjy,ak->ajy", layered_rows[0], layered_rows[1], inner_cos, -inner_sin
    )
    last_real, last_imag = rotate(
        last_real, last_imag, twist_cos.T[:, :, None], -twist_sin.T[:, :, None]
    )
    image_out = jnp.einsum("ajy,bj->yba", last_real, outer_cos, precision=HIGHEST) + jnp.einsum(
        "ajy,bj->yba", last_imag, outer_sin, precision=HIGHEST
    )
    image_out = image_out.reshape(TERMS, sub, chans, cols).transpose(2, 0, 1, 3) / PIX
    tiles = lax.all_to_all(image_out, "chan", split_axis=0, concat_axis=0, tiled=True)
    return tiles.transpose(1, 0, 2, 3).reshape(TERMS, rows, cols)


CHUNKS = 4
GROUP = 8
MESH = pl.DeviceIdType.MESH


def lane_tables(slabs, chans, sub):
    j = np.arange(chans)[:, None, None, None]
    v0 = np.arange(slabs)[None, :, None, None]
    r = np.arange(sub)[None, None, :, None]
    k = np.arange(sub)[None, None, None, :]
    phase = ((chans * r + j) * (v0 + slabs * k)) % PIX
    cos = np.cos(2.0 * np.pi * phase / PIX) / PIX
    sin = -np.sin(2.0 * np.pi * phase / PIX) / PIX
    top = np.concatenate([cos, sin], axis=3)
    low = np.concatenate([-sin, cos], axis=3)
    table = np.concatenate([top, low], axis=2).reshape(chans * slabs, 2 * sub, 2 * sub)
    table = table.astype(np.float32)
    high = table.astype(jnp.bfloat16)
    return high, (table - high.astype(np.float32)).astype(jnp.bfloat16)


def column_tables(slabs, chans, span):
    u1 = np.arange(span).reshape(slabs, CHUNKS, span // (slabs * CHUNKS))
    u1 = u1.transpose(1, 0, 2).reshape(span, 1)
    angle = 2.0 * np.pi * ((u1 * np.arange(span)[None, :]) % span) / span
    table = np.concatenate([np.cos(angle), np.sin(angle)], axis=1).astype(np.float32)
    high = table.astype(jnp.bfloat16)
    low = (table - high.astype(np.float32)).astype(jnp.bfloat16)
    turn = 2.0 * np.pi * np.arange(chans)[:, None] * np.arange(span)[None, :] / PIX
    turn = np.stack([np.cos(turn), np.sin(turn)], axis=1).reshape(2 * chans, span)
    return high, low, turn.astype(np.float32)


def sort_table(slabs, sub):
    span = slabs * sub
    source = jnp.arange(2 * span, dtype=jnp.int32)
    part, v = source // span, source % span
    target = (v % slabs) * (2 * sub) + part * sub + v // slabs
    return (target[:, None] == jnp.arange(2 * span, dtype=jnp.int32)[None, :]).astype(jnp.bfloat16)


def middle_kernel(
    slabs, chans, m_ref, vis_ref, wt_ref, off_ref, rs_ref, high_ref, low_ref, sort_ref,
    xhigh_ref, xlow_ref, turn_ref, out_ref,
    stage, xsend, xrecv, ohigh, olow, acc, rsend, rrecv, g_ref, q_ref, zin, mix, spec, back, landed, qsend, offs, work, vsort, wsort,
    z_send, z_recv, c_send, c_recv, b_send, b_recv, q_send, q_recv, o_send, o_recv,
    x_send, x_recv, r_send, r_recv,
):
    slab = lax.axis_index("slab")
    chan = lax.axis_index("chan")
    unit = g_ref.shape[3]
    lanes = g_ref.shape[4]
    half = lanes // 2
    span = slabs * half

    def slab_peer(d):
        return lax.rem(slab + d, slabs)

    def slab_from(d):
        return lax.rem(slab + slabs - d, slabs)

    def chan_peer(d):
        return lax.rem(chan + d, chans)

    def chan_from(d):
        return lax.rem(chan + chans - d, chans)

    def z_copy(c, d, owner):
        return pltpu.make_async_remote_copy(
            src_ref=g_ref.at[c, slab_peer(d)], dst_ref=zin.at[c, owner],
            send_sem=z_send.at[c, d], recv_sem=z_recv.at[c, d],
            device_id=(chan, slab_peer(d)), device_id_type=MESH)

    def c_copy(c, d, owner):
        return pltpu.make_async_remote_copy(
            src_ref=mix.at[c, d - 1], dst_ref=spec.at[c, owner],
            send_sem=c_send.at[c, d], recv_sem=c_recv.at[c, d],
            device_id=(chan_peer(d), slab), device_id_type=MESH)

    def b_copy(c, d, owner):
        return pltpu.make_async_remote_copy(
            src_ref=back.at[c, d - 1], dst_ref=landed.at[c, owner],
            send_sem=b_send.at[c, d], recv_sem=b_recv.at[c, d],
            device_id=(chan_peer(d), slab), device_id_type=MESH)

    def q_copy(c, d, owner):
        return pltpu.make_async_remote_copy(
            src_ref=qsend.at[c, slab_peer(d)], dst_ref=q_ref.at[c, owner],
            send_sem=q_send.at[c, d], recv_sem=q_recv.at[c, d],
            device_id=(chan, slab_peer(d)), device_id_type=MESH)

    def o_copy(d, owner):
        return pltpu.make_async_remote_copy(
            src_ref=off_ref, dst_ref=offs.at[owner],
            send_sem=o_send.at[d], recv_sem=o_recv.at[d],
            device_id=(chan_peer(d), slab), device_id_type=MESH)

    def x_copy(d, owner):
        return pltpu.make_async_remote_copy(
            src_ref=xsend.at[chan_peer(d)], dst_ref=xrecv.at[owner],
            send_sem=x_send.at[d], recv_sem=x_recv.at[d],
            device_id=(chan_peer(d), slab), device_id_type=MESH)

    def r_copy(d, owner):
        return pltpu.make_async_remote_copy(
            src_ref=rsend.at[chan_peer(d)], dst_ref=rrecv.at[owner],
            send_sem=r_send.at[d], recv_sem=r_recv.at[d],
            device_id=(chan_peer(d), slab), device_id_type=MESH)

    sub = half
    cols = m_ref.shape[2]
    quarter = unit // chans
    for m in range(TERMS):
        for q in range(cols // lanes):
            at = pl.ds(q * lanes, lanes)
            stage[q, m] = m_ref[m, :, at]
            for j in range(chans):
                xsend[j, m, :, at] = stage[q, m, pl.ds(j, sub, stride=chans), :]

    barrier = pltpu.get_barrier_semaphore()
    for d in range(1, slabs):
        pl.semaphore_signal(barrier, inc=1, device_id=(chan, slab_peer(d)), device_id_type=MESH)
    for d in range(1, chans):
        pl.semaphore_signal(barrier, inc=1, device_id=(chan_peer(d), slab), device_id_type=MESH)
    pl.semaphore_wait(barrier, slabs + chans - 2)

    for d in range(1, chans):
        x_copy(d, chan).start()
    for d in range(1, chans):
        o_copy(d, chan).start()

    offs[chan] = off_ref[...]
    xrecv[chan] = xsend[chan]
    acc[...] = jnp.zeros_like(acc)

    @pl.loop(0, CHUNKS)
    def _(c):
        rows = pl.ds(pl.multiple_of(c * unit, unit), unit)
        for jj in range(chans):
            at = pl.ds(jj * span, span)
            pair = jnp.concatenate([vis_ref[0, rows, at], vis_ref[1, rows, at]], axis=1)
            vsort[c, jj] = jnp.dot(pair, sort_ref[...], preferred_element_type=jnp.float32)
            pair = jnp.concatenate([wt_ref[rows, at], wt_ref[rows, at]], axis=1)
            wsort[c, jj] = jnp.dot(pair, sort_ref[...], preferred_element_type=jnp.float32)

    for d in range(1, chans):
        o_copy(d, chan_from(d)).wait_recv()

    for d in range(1, chans):
        x_copy(d, chan_from(d)).wait_recv()

    def halves(x):
        high = x.astype(jnp.bfloat16)
        return high, (x - high.astype(jnp.float32)).astype(jnp.bfloat16)

    for m in range(TERMS):
        @pl.loop(0, sub // 16)
        def _(i):
            start = pl.multiple_of(i * 16, 16)
            x = [xrecv[c, m, pl.ds(start, 16), :] for c in range(chans)]
            s0, s1, t0, t1 = x[0] + x[2], x[0] - x[2], x[1] + x[3], x[1] - x[3]
            for u0 in range(chans):
                cos, sin = turn_ref[2 * u0 : 2 * u0 + 1, :], turn_ref[2 * u0 + 1 : 2 * u0 + 2, :]
                if u0 % 2 == 0:
                    zr = s0 + t0 if u0 == 0 else s0 - t0
                    real, imag = zr * cos, -(zr * sin)
                else:
                    zi = -t1 if u0 == 1 else t1
                    real, imag = s1 * cos + zi * sin, zi * cos - s1 * sin
                one = pl.ds(pl.multiple_of(m * lanes + i * 16, 16), 16)
                two = pl.ds(pl.multiple_of(m * lanes + half + i * 16, 16), 16)
                left, right = pl.ds(0, cols), pl.ds(cols, cols)
                rh, rl = halves(real)
                ih, il = halves(imag)
                for into, re, im in ((ohigh, rh, ih), (olow, rl, il)):
                    into[u0, one, left] = re
                    into[u0, one, right] = im
                    into[u0, two, left] = im
                    into[u0, two, right] = -re

    @pl.loop(0, CHUNKS)
    def _(c):
        at = pl.ds(pl.multiple_of(c * slabs * quarter, slabs * quarter), slabs * quarter)
        th, tl = xhigh_ref[at, :], xlow_ref[at, :]
        dot = functools.partial(
            lax.dot_general, dimension_numbers=(((1,), (1,)), ((), ())),
            preferred_element_type=jnp.float32)
        for u0 in range(chans):
            found = dot(th, ohigh[u0]) + (dot(tl, ohigh[u0]) + dot(th, olow[u0]))
            for s in range(slabs):
                for m in range(TERMS):
                    g_ref[c, s, m, pl.ds(u0, quarter, stride=chans), :] = found[
                        s * quarter : (s + 1) * quarter, m * lanes : (m + 1) * lanes
                    ]
        for d in range(1, slabs):
            z_copy(c, d, slab).start()
        zin[c, slab] = g_ref[c, slab]

    lane = lax.broadcasted_iota(jnp.int32, (GROUP, lanes), 1)
    sign = jnp.where(lane < half, -1.0, 1.0)

    def times_i(x, direction):
        return pltpu.roll(x, half, 1) * (sign * direction)

    def four(x0, x1, x2, x3, direction):
        s0, s1, t0, t1 = x0 + x2, x0 - x2, x1 + x3, times_i(x1 - x3, direction)
        return s0 + t0, s1 + t1, s0 - t0, s1 - t1

    def eight(x, direction):
        root = math.sqrt(0.5)
        even = four(x[0], x[2], x[4], x[6], direction)
        odd = four(x[1], x[3], x[5], x[7], direction)
        odd = (
            odd[0],
            (odd[1] + times_i(odd[1], direction)) * root,
            times_i(odd[2], direction),
            (times_i(odd[3], direction) - odd[3]) * root,
        )
        return [e + o for e, o in zip(even, odd)] + [e - o for e, o in zip(even, odd)]

    def split(x):
        high = x.astype(jnp.bfloat16)
        return high, (x - high.astype(jnp.float32)).astype(jnp.bfloat16)

    def product(x, t, dims):
        high, low = split(x)
        dot = functools.partial(
            lax.dot_general, dimension_numbers=(dims, ((), ())),
            preferred_element_type=jnp.float32)
        wide = dot(high, high_ref[t])
        return wide + (dot(low, high_ref[t]) + dot(high, low_ref[t]))

    def spread(c):
        for d in range(1, slabs):
            z_copy(c, d, slab_from(d)).wait_recv()

        @pl.loop(0, slabs)
        def _(s):
            base, slope = zin[c, s, 0], zin[c, s, 1]
            spec[c, chan, s] = base + offs[chan][0:1, :] * slope
            for d in range(1, chans):
                mix[c, d - 1, s] = base + offs[chan_peer(d)][0:1, :] * slope

        for d in range(1, chans):
            c_copy(c, d, chan).start()

    def weigh(c):
        for d in range(1, chans):
            c_copy(c, d, chan_from(d)).wait_recv()
        damping = rs_ref[0:1, :]

        @pl.loop(0, unit // GROUP)
        def _(i):
            rows = pl.ds(pl.multiple_of(i * GROUP, GROUP), GROUP)
            for j in range(chans):
                out = eight([spec[c, j, s, rows, :] for s in range(slabs)], -1.0)
                for v0 in range(slabs):
                    work[j * slabs + v0, rows, :] = out[v0]

        @pl.loop(0, chans * slabs)
        def _(t):
            work[t] = product(work[t], t, ((1,), (0,)))

        @pl.loop(0, unit // GROUP)
        def _(i):
            rows = pl.ds(pl.multiple_of(i * GROUP, GROUP), GROUP)
            for v0 in range(slabs):
                at = pl.ds(v0 * lanes, lanes)
                found = four(*[work[j * slabs + v0, rows, :] for j in range(chans)], -1.0)
                kept = []
                for jj in range(chans):
                    delta = vsort[c, jj, rows, at] - wsort[c, jj, rows, at] * found[jj]
                    power = delta * delta
                    power = power + pltpu.roll(power, half, 1)
                    kept.append(delta / (1.0 + damping * power))
                out = four(*kept, 1.0)
                for j in range(chans):
                    work[j * slabs + v0, rows, :] = out[j]

        @pl.loop(0, chans * slabs)
        def _(t):
            work[t] = product(work[t], t, ((1,), (1,)))

        @pl.loop(0, unit // GROUP)
        def _(i):
            rows = pl.ds(pl.multiple_of(i * GROUP, GROUP), GROUP)
            for d in range(chans):
                first = chan_peer(d) * slabs
                out = eight([work[first + v0, rows, :] for v0 in range(slabs)], 1.0)
                for s in range(slabs):
                    if d == 0:
                        landed[c, chan, s, rows, :] = out[s]
                    else:
                        back[c, d - 1, s, rows, :] = out[s]

        for d in range(1, chans):
            b_copy(c, d, chan).start()

    def gather(c):
        for d in range(1, chans):
            b_copy(c, d, chan_from(d)).wait_recv()

        @pl.loop(0, slabs)
        def _(s):
            parts = [landed[c, j, s] for j in range(chans)]
            qsend[c, s, 0] = (parts[0] + parts[1]) + (parts[2] + parts[3])
            scaled = [parts[j] * offs[j][0:1, :] for j in range(chans)]
            qsend[c, s, 1] = (scaled[0] + scaled[1]) + (scaled[2] + scaled[3])

        q_ref[c, slab] = qsend[c, slab]
        for d in range(1, slabs):
            q_copy(c, d, slab).start()

    def finish(c):
        for d in range(1, slabs):
            q_copy(c, d, slab_from(d)).wait_recv()
        at = pl.ds(pl.multiple_of(c * slabs * quarter, slabs * quarter), slabs * quarter)
        th, tl = xhigh_ref[at, :], xlow_ref[at, :]
        dot = functools.partial(jnp.dot, preferred_element_type=jnp.float32)
        for u0 in range(chans):
            held = jnp.concatenate(
                [
                    jnp.concatenate(
                        [
                            q_ref[c, s, t, pl.ds(u0, quarter, stride=chans), :]
                            for t in range(TERMS)
                        ],
                        axis=1,
                    )
                    for s in range(slabs)
                ],
                axis=0,
            )
            qh, ql = halves(held.T)
            acc[u0] += dot(qh, th) + (dot(ql, th) + dot(qh, tl))

    @pl.loop(0, CHUNKS + 4)
    def _(step):
        @pl.when(step < CHUNKS)
        def _():
            spread(step)

        @pl.when(jnp.logical_and(step >= 1, step < CHUNKS + 1))
        def _():
            weigh(step - 1)

        @pl.when(jnp.logical_and(step >= 3, step < CHUNKS + 3))
        def _():
            gather(step - 3)

        @pl.when(step >= 4)
        def _():
            finish(step - 4)

    for t in range(TERMS):
        @pl.loop(0, sub // GROUP)
        def _(i):
            rows = pl.ds(pl.multiple_of(i * GROUP, GROUP), GROUP)
            one = pl.ds(pl.multiple_of(t * lanes + i * GROUP, GROUP), GROUP)
            two = pl.ds(pl.multiple_of(t * lanes + half + i * GROUP, GROUP), GROUP)
            left, right = pl.ds(0, cols), pl.ds(cols, cols)
            real, imag = [], []
            for u0 in range(chans):
                cos, sin = turn_ref[2 * u0 : 2 * u0 + 1, :], turn_ref[2 * u0 + 1 : 2 * u0 + 2, :]
                yr = acc[u0, one, left] - acc[u0, two, right]
                yi = acc[u0, one, right] + acc[u0, two, left]
                real.append(yr * cos - yi * sin)
                imag.append(yr * sin + yi * cos)
            e0, e1 = real[0] + real[2], real[0] - real[2]
            o0, o1 = real[1] + real[3], imag[3] - imag[1]
            rsend[0, t, rows, :] = e0 + o0
            rsend[1, t, rows, :] = e1 + o1
            rsend[2, t, rows, :] = e0 - o0
            rsend[3, t, rows, :] = e1 - o1

    for d in range(1, chans):
        r_copy(d, chan).start()
    rrecv[chan] = rsend[chan]
    for d in range(1, chans):
        r_copy(d, chan_from(d)).wait_recv()
    for t in range(TERMS):
        for q in range(cols // lanes):
            at = pl.ds(q * lanes, lanes)
            for j in range(chans):
                stage[q, t, pl.ds(j, sub, stride=chans), :] = rrecv[j, t, :, at]
            out_ref[t, :, at] = stage[q, t]

    @pl.loop(0, CHUNKS)
    def _(c):
        for d in range(1, slabs):
            q_copy(c, d, slab).wait_send()
            z_copy(c, d, slab).wait_send()
        for d in range(1, chans):
            c_copy(c, d, chan).wait_send()
            b_copy(c, d, chan).wait_send()

    for d in range(1, chans):
        o_copy(d, chan).wait_send()
        x_copy(d, chan).wait_send()
        r_copy(d, chan).wait_send()


def local(taylor_models, gridded_vis, uv_weight, freq_ratio, robust_scale):
    chans = lax.axis_size("chan")
    slabs = lax.axis_size("slab")
    rows = taylor_models.shape[1]
    cols = taylor_models.shape[2]
    sub = rows // chans
    if slabs != 8 or chans != 4 or 2 * sub != 128:
        return local_general(taylor_models, gridded_vis, uv_weight, freq_ratio, robust_scale)
    unit = PIX // slabs // CHUNKS
    lanes = 2 * sub
    high, low = lane_tables(slabs, chans, sub)
    xhigh, xlow, turn = column_tables(slabs, chans, cols)
    vmem = pl.BlockSpec(memory_space=pltpu.VMEM)
    f32 = jnp.float32
    tile = (unit, lanes)
    piece = pltpu.VMEM((chans, TERMS, sub, cols), f32)
    operand = pltpu.VMEM((chans, TERMS * lanes, 2 * cols), jnp.bfloat16)
    columns = pltpu.VMEM((CHUNKS, slabs, TERMS) + tile, f32)
    wide = pltpu.VMEM((CHUNKS, chans, slabs) + tile, f32)
    others = pltpu.VMEM((CHUNKS, chans - 1, slabs) + tile, f32)
    sorted_tiles = pltpu.VMEM((CHUNKS, chans, unit, slabs * lanes), f32)
    return pl.pallas_call(
        functools.partial(middle_kernel, slabs, chans),
        out_shape=jax.ShapeDtypeStruct((TERMS, rows, cols), f32),
        in_specs=[vmem] * 11,
        out_specs=vmem,
        scratch_shapes=[
            pltpu.VMEM((cols // lanes, TERMS, rows, lanes), f32),
            piece, piece, operand, operand,
            pltpu.VMEM((chans, TERMS * lanes, 2 * cols), f32),
            piece, piece, columns, columns,
            columns, others, wide, others, wide, columns,
            pltpu.VMEM((chans, 8, lanes), f32),
            pltpu.VMEM((chans * slabs,) + tile, f32),
            sorted_tiles, sorted_tiles,
        ]
        + [pltpu.SemaphoreType.DMA((CHUNKS, slabs))] * 2
        + [pltpu.SemaphoreType.DMA((CHUNKS, chans))] * 4
        + [pltpu.SemaphoreType.DMA((CHUNKS, slabs))] * 2
        + [pltpu.SemaphoreType.DMA((chans,))] * 6,
        compiler_params=pltpu.CompilerParams(
            collective_id=0, has_side_effects=True, vmem_limit_bytes=63 * 1024 * 1024
        ),
    )(
        taylor_models, gridded_vis[0], uv_weight[0],
        jnp.broadcast_to(freq_ratio[0] - 1.0, (8, lanes)),
        jnp.broadcast_to(robust_scale[0], (8, lanes)),
        jnp.asarray(high), jnp.asarray(low), sort_table(slabs, sub),
        jnp.asarray(xhigh), jnp.asarray(xlow), jnp.asarray(turn),
    )


def solution(mesh):
    placed = (
        P(None, "slab", "chan"),
        P("chan", None, "slab", None),
        P("chan", "slab", None),
        P("chan"),
        P("chan"),
    )
    return jax.shard_map(
        local, mesh=mesh, in_specs=placed, out_specs=P(None, "slab", "chan"), check_vma=False
    )
```

```python
import functools
import math

import jax
import jax.numpy as jnp
import numpy as np
from jax import lax
from jax.experimental import pallas as pl
from jax.experimental.pallas import tpu as pltpu
from jax.sharding import PartitionSpec as P

PIX = 2048
TERMS = 2


HIGHEST = lax.Precision.HIGH


def dft_table(points, direction):
    steps_all = jnp.arange(points, dtype=jnp.int32)
    product = steps_all[:, None] * steps_all[None, :] % points
    angles = product.astype(jnp.float32) * (2.0 * math.pi / points)
    return (jnp.cos(angles), direction * jnp.sin(angles))


def twiddle_table(outer_points, inner_points, direction):
    outer_steps = jnp.arange(outer_points, dtype=jnp.int32)
    inner_steps = jnp.arange(inner_points, dtype=jnp.int32)
    overall = outer_points * inner_points
    product = outer_steps[:, None] * inner_steps[None, :] % overall
    angles = product.astype(jnp.float32) * (2.0 * math.pi / overall)
    return (jnp.cos(angles), direction * jnp.sin(angles))


def complex_product(formula, left_real, left_imag, table_real, table_imag):
    out_real = jnp.einsum(formula, left_real, table_real, precision=HIGHEST) - jnp.einsum(
        formula, left_imag, table_imag, precision=HIGHEST
    )
    out_imag = jnp.einsum(formula, left_real, table_imag, precision=HIGHEST) + jnp.einsum(
        formula, left_imag, table_real, precision=HIGHEST
    )
    return (out_real, out_imag)


def rotate(left_real, left_imag, table_real, table_imag):
    return (
        left_real * table_real - left_imag * table_imag,
        left_real * table_imag + left_imag * table_real,
    )


def local_general(taylor_models, gridded_vis, uv_weight, freq_ratio, robust_scale):
    inner_count = 128
    outer_count = PIX // inner_count
    chans = lax.axis_size("chan")
    slabs = lax.axis_size("slab")
    rows = taylor_models.shape[1]
    cols = taylor_models.shape[2]
    sub = rows // chans
    col_count = PIX // slabs
    outer_cos, outer_sin = dft_table(outer_count, -1.0)
    inner_cos, inner_sin = dft_table(inner_count, -1.0)
    twist_cos, twist_sin = twiddle_table(outer_count, inner_count, -1.0)
    offsets = lax.all_gather(freq_ratio, "chan", axis=0, tiled=True) - 1.0

    pieces = taylor_models.reshape(TERMS, chans, sub, cols).transpose(1, 0, 2, 3)
    pieces = lax.all_to_all(pieces, "chan", split_axis=0, concat_axis=0, tiled=True)
    layered = pieces.transpose(1, 2, 0, 3).reshape(TERMS * sub, outer_count, inner_count)
    part_real = jnp.einsum("yba,jb->yja", layered, outer_cos, precision=HIGHEST)
    part_imag = jnp.einsum("yba,jb->yja", layered, outer_sin, precision=HIGHEST)
    turned_real, turned_imag = rotate(part_real, part_imag, twist_cos, twist_sin)
    spec_real, spec_imag = complex_product(
        "yja,ka->kjy", turned_real, turned_imag, inner_cos, inner_sin
    )
    outgoing = jnp.stack(
        [
            spec_real.reshape(slabs, col_count, TERMS * sub),
            spec_imag.reshape(slabs, col_count, TERMS * sub),
        ],
        axis=1,
    )
    arrived = lax.all_to_all(outgoing, "slab", split_axis=0, concat_axis=0, tiled=True)
    arrived = arrived.reshape(slabs, 2, col_count, TERMS, sub)
    arrived = arrived.transpose(3, 1, 2, 0, 4).reshape(TERMS, 2, col_count, slabs * sub)
    mixed = arrived[0][None] + offsets[:, None, None, None] * arrived[1][None]
    mixed = lax.all_to_all(mixed, "chan", split_axis=0, concat_axis=0, tiled=True)
    columns = mixed.reshape(chans, 2, col_count, slabs, sub).transpose(1, 2, 3, 0, 4)
    layered_cols = columns.reshape(2, col_count, outer_count, inner_count)
    part_real, part_imag = complex_product(
        "uba,jb->uja", layered_cols[0], layered_cols[1], outer_cos, outer_sin
    )
    turned_real, turned_imag = rotate(part_real, part_imag, twist_cos, twist_sin)
    freq_real, freq_imag = complex_product(
        "uja,ka->ujk", turned_real, turned_imag, inner_cos, inner_sin
    )
    freq_real = freq_real / PIX
    freq_imag = freq_imag / PIX
    weight = (
        uv_weight[0]
        .astype(jnp.float32)
        .reshape(col_count, inner_count, outer_count)
        .transpose(0, 2, 1)
    )
    visible = (
        gridded_vis[0]
        .astype(jnp.float32)
        .reshape(2, col_count, inner_count, outer_count)
        .transpose(0, 1, 3, 2)
    )
    delta_real = visible[0] - weight * freq_real
    delta_imag = visible[1] - weight * freq_imag
    robust = 1.0 / (1.0 + robust_scale[0] * (delta_real * delta_real + delta_imag * delta_imag))
    weighted_real = robust * delta_real
    weighted_imag = robust * delta_imag
    back_real, back_imag = complex_product(
        "ujk,ak->uja", weighted_real, weighted_imag, inner_cos, -inner_sin
    )
    back_real, back_imag = rotate(back_real, back_imag, twist_cos, -twist_sin)
    back_real, back_imag = complex_product(
        "uja,bj->uba", back_real, back_imag, outer_cos, -outer_sin
    )
    back = jnp.stack([back_real, back_imag]).reshape(2, col_count, slabs, chans, sub)
    back = back.transpose(3, 0, 1, 2, 4).reshape(chans, 2, col_count, slabs * sub)
    back = lax.all_to_all(back, "chan", split_axis=0, concat_axis=0, tiled=True)
    total = jnp.stack(
        [jnp.sum(back * offsets[:, None, None, None] ** t, axis=0) for t in range(TERMS)]
    )
    total = total.reshape(TERMS, 2, col_count, slabs, sub).transpose(3, 1, 2, 0, 4)
    total = total.reshape(slabs, 2, col_count, TERMS * sub)
    total = lax.all_to_all(total, "slab", split_axis=0, concat_axis=0, tiled=True)
    layered_rows = total.transpose(1, 0, 2, 3).reshape(2, inner_count, outer_count, TERMS * sub)
    last_real, last_imag = complex_product(
        "kjy,ak->ajy", layered_rows[0], layered_rows[1], inner_cos, -inner_sin
    )
    last_real, last_imag = rotate(
        last_real, last_imag, twist_cos.T[:, :, None], -twist_sin.T[:, :, None]
    )
    image_out = jnp.einsum("ajy,bj->yba", last_real, outer_cos, precision=HIGHEST) + jnp.einsum(
        "ajy,bj->yba", last_imag, outer_sin, precision=HIGHEST
    )
    image_out = image_out.reshape(TERMS, sub, chans, cols).transpose(2, 0, 1, 3) / PIX
    tiles = lax.all_to_all(image_out, "chan", split_axis=0, concat_axis=0, tiled=True)
    return tiles.transpose(1, 0, 2, 3).reshape(TERMS, rows, cols)


CHUNKS = 4
GROUP = 8
MESH = pl.DeviceIdType.MESH


def lane_tables(slabs, chans, sub):
    j = np.arange(chans)[:, None, None, None]
    v0 = np.arange(slabs)[None, :, None, None]
    r = np.arange(sub)[None, None, :, None]
    k = np.arange(sub)[None, None, None, :]
    phase = ((chans * r + j) * (v0 + slabs * k)) % PIX
    cos = np.cos(2.0 * np.pi * phase / PIX) / PIX
    sin = -np.sin(2.0 * np.pi * phase / PIX) / PIX
    top = np.concatenate([cos, sin], axis=3)
    low = np.concatenate([-sin, cos], axis=3)
    table = np.concatenate([top, low], axis=2).reshape(chans * slabs, 2 * sub, 2 * sub)
    table = table.astype(np.float32)
    high = table.astype(jnp.bfloat16)
    return high, (table - high.astype(np.float32)).astype(jnp.bfloat16)


def column_tables(slabs, chans, span):
    u1 = np.arange(span).reshape(slabs, CHUNKS, span // (slabs * CHUNKS))
    u1 = u1.transpose(1, 0, 2).reshape(span, 1)
    angle = 2.0 * np.pi * ((u1 * np.arange(span)[None, :]) % span) / span
    table = np.concatenate([np.cos(angle), np.sin(angle)], axis=1).astype(np.float32)
    high = table.astype(jnp.bfloat16)
    low = (table - high.astype(np.float32)).astype(jnp.bfloat16)
    turn = 2.0 * np.pi * np.arange(chans)[:, None] * np.arange(span)[None, :] / PIX
    turn = np.stack([np.cos(turn), np.sin(turn)], axis=1).reshape(2 * chans, span)
    parts = [x.reshape(CHUNKS, span // CHUNKS, 2 * span) for x in (high, low)]
    return np.stack(parts, axis=1).reshape(2 * span, 2 * span), turn.astype(np.float32)


def sort_table(slabs, sub):
    source = jnp.arange(slabs * sub, dtype=jnp.int32)
    target = (source % slabs) * sub + source // slabs
    return (target[:, None] == source[None, :]).astype(jnp.bfloat16)


def middle_kernel(
    slabs, chans, m_ref, vis_ref, wt_ref, off_ref, rs_ref, high_ref, low_ref, sort_ref,
    xtab_ref, turn_ref, out_ref,
    stage, xsend, xrecv, ohigh, olow, acc, rsend, rrecv, g_ref, q_ref, zin, mix, spec, back, landed, qsend, offs, work, vsort, wsort,
    z_send, z_recv, c_send, c_recv, b_send, b_recv, q_send, q_recv, o_send, o_recv,
    x_send, x_recv, r_send, r_recv,
):
    slab = lax.axis_index("slab")
    chan = lax.axis_index("chan")
    unit = g_ref.shape[3]
    lanes = g_ref.shape[4]
    half = lanes // 2
    span = slabs * half

    def slab_peer(d):
        return lax.rem(slab + d, slabs)

    def slab_from(d):
        return lax.rem(slab + slabs - d, slabs)

    def chan_peer(d):
        return lax.rem(chan + d, chans)

    def chan_from(d):
        return lax.rem(chan + chans - d, chans)

    def z_copy(c, d, owner):
        return pltpu.make_async_remote_copy(
            src_ref=g_ref.at[c, slab_peer(d)], dst_ref=zin.at[c, owner],
            send_sem=z_send.at[c, d], recv_sem=z_recv.at[c, d],
            device_id=(chan, slab_peer(d)), device_id_type=MESH)

    def c_copy(c, d, owner):
        return pltpu.make_async_remote_copy(
            src_ref=mix.at[c, d - 1], dst_ref=spec.at[c, owner],
            send_sem=c_send.at[c, d], recv_sem=c_recv.at[c, d],
            device_id=(chan_peer(d), slab), device_id_type=MESH)

    def b_copy(c, d, owner):
        return pltpu.make_async_remote_copy(
            src_ref=back.at[c, d - 1], dst_ref=landed.at[c, owner],
            send_sem=b_send.at[c, d], recv_sem=b_recv.at[c, d],
            device_id=(chan_peer(d), slab), device_id_type=MESH)

    def q_copy(c, d, owner):
        return pltpu.make_async_remote_copy(
            src_ref=qsend.at[c, slab_peer(d)], dst_ref=q_ref.at[c, owner],
            send_sem=q_send.at[c, d], recv_sem=q_recv.at[c, d],
            device_id=(chan, slab_peer(d)), device_id_type=MESH)

    def o_copy(d, owner):
        return pltpu.make_async_remote_copy(
            src_ref=off_ref, dst_ref=offs.at[owner],
            send_sem=o_send.at[d], recv_sem=o_recv.at[d],
            device_id=(chan_peer(d), slab), device_id_type=MESH)

    def x_copy(d, owner):
        return pltpu.make_async_remote_copy(
            src_ref=xsend.at[chan_peer(d)], dst_ref=xrecv.at[owner],
            send_sem=x_send.at[d], recv_sem=x_recv.at[d],
            device_id=(chan_peer(d), slab), device_id_type=MESH)

    def r_copy(d, owner):
        return pltpu.make_async_remote_copy(
            src_ref=rsend.at[chan_peer(d)], dst_ref=rrecv.at[owner],
            send_sem=r_send.at[d], recv_sem=r_recv.at[d],
            device_id=(chan_peer(d), slab), device_id_type=MESH)

    sub = half
    cols = m_ref.shape[2]
    quarter = unit // chans
    for m in range(TERMS):
        for q in range(cols // lanes):
            at = pl.ds(q * lanes, lanes)
            stage[q, m] = m_ref[m, :, at]
            for j in range(chans):
                xsend[j, m, :, at] = stage[q, m, pl.ds(j, sub, stride=chans), :]

    barrier = pltpu.get_barrier_semaphore()
    for d in range(1, slabs):
        pl.semaphore_signal(barrier, inc=1, device_id=(chan, slab_peer(d)), device_id_type=MESH)
    for d in range(1, chans):
        pl.semaphore_signal(barrier, inc=1, device_id=(chan_peer(d), slab), device_id_type=MESH)
    pl.semaphore_wait(barrier, slabs + chans - 2)

    for d in range(1, chans):
        x_copy(d, chan).start()
    for d in range(1, chans):
        o_copy(d, chan).start()

    offs[chan] = off_ref[...]
    xrecv[chan] = xsend[chan]
    acc[...] = jnp.zeros_like(acc)

    @pl.loop(0, chans)
    def _(jj):
        at = pl.ds(pl.multiple_of(jj * span, span), span)
        dot = functools.partial(jnp.dot, preferred_element_type=jnp.float32)
        real, imag = dot(vis_ref[0, :, at], sort_ref[...]), dot(vis_ref[1, :, at], sort_ref[...])
        scale = dot(wt_ref[:, at], sort_ref[...])
        lower = lax.broadcasted_iota(jnp.int32, (unit, lanes), 1) < half
        for c in range(CHUNKS):
            for p in range(slabs // 2):
                re, im, wt = [
                    x[c * unit : (c + 1) * unit, p * lanes : (p + 1) * lanes]
                    for x in (real, imag, scale)
                ]
                even, odd = pl.ds(2 * p * lanes, lanes), pl.ds((2 * p + 1) * lanes, lanes)
                turned = pltpu.roll(wt, half, 1)
                vsort[c, jj, :, even] = jnp.where(lower, re, pltpu.roll(im, half, 1))
                vsort[c, jj, :, odd] = jnp.where(lower, pltpu.roll(re, half, 1), im)
                wsort[c, jj, :, even] = jnp.where(lower, wt, turned)
                wsort[c, jj, :, odd] = jnp.where(lower, turned, wt)

    for d in range(1, chans):
        o_copy(d, chan_from(d)).wait_recv()

    for d in range(1, chans):
        x_copy(d, chan_from(d)).wait_recv()

    def halves(x):
        high = x.astype(jnp.bfloat16)
        return high, (x - high.astype(jnp.float32)).astype(jnp.bfloat16)

    for m in range(TERMS):
        @pl.loop(0, sub // 16)
        def _(i):
            start = pl.multiple_of(i * 16, 16)
            x = [xrecv[c, m, pl.ds(start, 16), :] for c in range(chans)]
            s0, s1, t0, t1 = x[0] + x[2], x[0] - x[2], x[1] + x[3], x[1] - x[3]
            for u0 in range(chans):
                cos, sin = turn_ref[2 * u0 : 2 * u0 + 1, :], turn_ref[2 * u0 + 1 : 2 * u0 + 2, :]
                if u0 % 2 == 0:
                    zr = s0 + t0 if u0 == 0 else s0 - t0
                    real, imag = zr * cos, -(zr * sin)
                else:
                    zi = -t1 if u0 == 1 else t1
                    real, imag = s1 * cos + zi * sin, zi * cos - s1 * sin
                one = pl.ds(pl.multiple_of(m * lanes + i * 16, 16), 16)
                two = pl.ds(pl.multiple_of(m * lanes + half + i * 16, 16), 16)
                left, right = pl.ds(0, cols), pl.ds(cols, cols)
                rh, rl = halves(real)
                ih, il = halves(imag)
                for into, re, im in ((ohigh, rh, ih), (olow, rl, il)):
                    into[u0, one, left] = re
                    into[u0, one, right] = im
                    into[u0, two, left] = im
                    into[u0, two, right] = -re

    @pl.loop(0, CHUNKS)
    def _(c):
        count = slabs * quarter
        at = pl.multiple_of(c * 2 * count, 2 * count)
        both, wide = xtab_ref[pl.ds(at, 2 * count), :], xtab_ref[pl.ds(at, count), :]
        dot = functools.partial(
            lax.dot_general, dimension_numbers=(((1,), (1,)), ((), ())),
            preferred_element_type=jnp.float32)
        for u0 in range(chans):
            found = dot(both, ohigh[u0])
            found = found[:count] + (found[count:] + dot(wide, olow[u0]))
            for s in range(slabs):
                for m in range(TERMS):
                    g_ref[c, s, m, pl.ds(u0, quarter, stride=chans), :] = found[
                        s * quarter : (s + 1) * quarter, m * lanes : (m + 1) * lanes
                    ]
        for d in range(1, slabs):
            z_copy(c, d, slab).start()
        zin[c, slab] = g_ref[c, slab]

    lane = lax.broadcasted_iota(jnp.int32, (GROUP, lanes), 1)
    sign = jnp.where(lane < half, -1.0, 1.0)

    def times_i(x, direction):
        return pltpu.roll(x, half, 1) * (sign * direction)

    def four(x0, x1, x2, x3, direction):
        s0, s1, t0, t1 = x0 + x2, x0 - x2, x1 + x3, times_i(x1 - x3, direction)
        return s0 + t0, s1 + t1, s0 - t0, s1 - t1

    def eight(x, direction):
        root = math.sqrt(0.5)
        even = four(x[0], x[2], x[4], x[6], direction)
        odd = four(x[1], x[3], x[5], x[7], direction)
        odd = (
            odd[0],
            (odd[1] + times_i(odd[1], direction)) * root,
            times_i(odd[2], direction),
            (times_i(odd[3], direction) - odd[3]) * root,
        )
        return [e + o for e, o in zip(even, odd)] + [e - o for e, o in zip(even, odd)]

    def split(x):
        high = x.astype(jnp.bfloat16)
        return high, (x - high.astype(jnp.float32)).astype(jnp.bfloat16)

    def product(x, t, dims):
        high, low = split(x)
        dot = functools.partial(
            lax.dot_general, dimension_numbers=(dims, ((), ())),
            preferred_element_type=jnp.float32)
        both = dot(jnp.concatenate([high, low], axis=0), high_ref[t])
        return both[:unit] + (both[unit:] + dot(high, low_ref[t]))

    def spread(c):
        for d in range(1, slabs):
            z_copy(c, d, slab_from(d)).wait_recv()

        @pl.loop(0, slabs)
        def _(s):
            base, slope = zin[c, s, 0], zin[c, s, 1]
            spec[c, chan, s] = base + offs[chan][0:1, :] * slope
            for d in range(1, chans):
                mix[c, d - 1, s] = base + offs[chan_peer(d)][0:1, :] * slope

        for d in range(1, chans):
            c_copy(c, d, chan).start()

    def weigh(c):
        for d in range(1, chans):
            c_copy(c, d, chan_from(d)).wait_recv()
        damping = rs_ref[0:1, :]

        @pl.loop(0, unit // GROUP)
        def _(i):
            rows = pl.ds(pl.multiple_of(i * GROUP, GROUP), GROUP)
            for j in range(chans):
                out = eight([spec[c, j, s, rows, :] for s in range(slabs)], -1.0)
                for v0 in range(slabs):
                    work[j * slabs + v0, rows, :] = out[v0]

        @pl.loop(0, chans)
        def _(j):
            tiles = [j * slabs + v0 for v0 in range(slabs)]
            done = [product(work[t], t, ((1,), (0,))) for t in tiles]
            for t, x in zip(tiles, done):
                work[t] = x

        @pl.loop(0, unit // GROUP)
        def _(i):
            rows = pl.ds(pl.multiple_of(i * GROUP, GROUP), GROUP)
            for v0 in range(slabs):
                at = pl.ds(v0 * lanes, lanes)
                found = four(*[work[j * slabs + v0, rows, :] for j in range(chans)], -1.0)
                kept = []
                for jj in range(chans):
                    delta = vsort[c, jj, rows, at] - wsort[c, jj, rows, at] * found[jj]
                    power = delta * delta
                    power = power + pltpu.roll(power, half, 1)
                    kept.append(delta / (1.0 + damping * power))
                out = four(*kept, 1.0)
                for j in range(chans):
                    work[j * slabs + v0, rows, :] = out[j]

        @pl.loop(0, chans)
        def _(j):
            tiles = [j * slabs + v0 for v0 in range(slabs)]
            done = [product(work[t], t, ((1,), (1,))) for t in tiles]
            for t, x in zip(tiles, done):
                work[t] = x

        @pl.loop(0, unit // GROUP)
        def _(i):
            rows = pl.ds(pl.multiple_of(i * GROUP, GROUP), GROUP)
            for d in range(chans):
                first = chan_peer(d) * slabs
                out = eight([work[first + v0, rows, :] for v0 in range(slabs)], 1.0)
                for s in range(slabs):
                    if d == 0:
                        landed[c, chan, s, rows, :] = out[s]
                    else:
                        back[c, d - 1, s, rows, :] = out[s]

        for d in range(1, chans):
            b_copy(c, d, chan).start()

    def gather(c):
        for d in range(1, chans):
            b_copy(c, d, chan_from(d)).wait_recv()

        @pl.loop(0, slabs)
        def _(s):
            parts = [landed[c, j, s] for j in range(chans)]
            qsend[c, s, 0] = (parts[0] + parts[1]) + (parts[2] + parts[3])
            scaled = [parts[j] * offs[j][0:1, :] for j in range(chans)]
            qsend[c, s, 1] = (scaled[0] + scaled[1]) + (scaled[2] + scaled[3])

        q_ref[c, slab] = qsend[c, slab]
        for d in range(1, slabs):
            q_copy(c, d, slab).start()

    def finish(c):
        for d in range(1, slabs):
            q_copy(c, d, slab_from(d)).wait_recv()
        count = slabs * quarter
        at = pl.multiple_of(c * 2 * count, 2 * count)
        th, tl = xtab_ref[pl.ds(at, count), :], xtab_ref[pl.ds(at + count, count), :]
        dot = functools.partial(jnp.dot, preferred_element_type=jnp.float32)
        for u0 in range(chans):
            held = jnp.concatenate(
                [
                    jnp.concatenate(
                        [
                            q_ref[c, s, t, pl.ds(u0, quarter, stride=chans), :]
                            for t in range(TERMS)
                        ],
                        axis=1,
                    )
                    for s in range(slabs)
                ],
                axis=0,
            )
            qh, ql = halves(held.T)
            found = dot(jnp.concatenate([qh, ql], axis=0), th)
            acc[u0] += found[: TERMS * lanes] + (found[TERMS * lanes :] + dot(qh, tl))

    @pl.loop(0, CHUNKS + 4)
    def _(step):
        @pl.when(step < CHUNKS)
        def _():
            spread(step)

        @pl.when(jnp.logical_and(step >= 1, step < CHUNKS + 1))
        def _():
            weigh(step - 1)

        @pl.when(jnp.logical_and(step >= 3, step < CHUNKS + 3))
        def _():
            gather(step - 3)

        @pl.when(step >= 4)
        def _():
            finish(step - 4)

    for t in range(TERMS):
        @pl.loop(0, sub // GROUP)
        def _(i):
            rows = pl.ds(pl.multiple_of(i * GROUP, GROUP), GROUP)
            one = pl.ds(pl.multiple_of(t * lanes + i * GROUP, GROUP), GROUP)
            two = pl.ds(pl.multiple_of(t * lanes + half + i * GROUP, GROUP), GROUP)
            left, right = pl.ds(0, cols), pl.ds(cols, cols)
            real, imag = [], []
            for u0 in range(chans):
                cos, sin = turn_ref[2 * u0 : 2 * u0 + 1, :], turn_ref[2 * u0 + 1 : 2 * u0 + 2, :]
                yr = acc[u0, one, left] - acc[u0, two, right]
                yi = acc[u0, one, right] + acc[u0, two, left]
                real.append(yr * cos - yi * sin)
                imag.append(yr * sin + yi * cos)
            e0, e1 = real[0] + real[2], real[0] - real[2]
            o0, o1 = real[1] + real[3], imag[3] - imag[1]
            rsend[0, t, rows, :] = e0 + o0
            rsend[1, t, rows, :] = e1 + o1
            rsend[2, t, rows, :] = e0 - o0
            rsend[3, t, rows, :] = e1 - o1

    for d in range(1, chans):
        r_copy(d, chan).start()
    rrecv[chan] = rsend[chan]
    for d in range(1, chans):
        r_copy(d, chan_from(d)).wait_recv()
    for t in range(TERMS):
        for q in range(cols // lanes):
            at = pl.ds(q * lanes, lanes)
            for j in range(chans):
                stage[q, t, pl.ds(j, sub, stride=chans), :] = rrecv[j, t, :, at]
            out_ref[t, :, at] = stage[q, t]

    @pl.loop(0, CHUNKS)
    def _(c):
        for d in range(1, slabs):
            q_copy(c, d, slab).wait_send()
            z_copy(c, d, slab).wait_send()
        for d in range(1, chans):
            c_copy(c, d, chan).wait_send()
            b_copy(c, d, chan).wait_send()

    for d in range(1, chans):
        o_copy(d, chan).wait_send()
        x_copy(d, chan).wait_send()
        r_copy(d, chan).wait_send()


def local(taylor_models, gridded_vis, uv_weight, freq_ratio, robust_scale):
    chans = lax.axis_size("chan")
    slabs = lax.axis_size("slab")
    rows = taylor_models.shape[1]
    cols = taylor_models.shape[2]
    sub = rows // chans
    if slabs != 8 or chans != 4 or 2 * sub != 128:
        return local_general(taylor_models, gridded_vis, uv_weight, freq_ratio, robust_scale)
    unit = PIX // slabs // CHUNKS
    lanes = 2 * sub
    high, low = lane_tables(slabs, chans, sub)
    xtab, turn = column_tables(slabs, chans, cols)
    vmem = pl.BlockSpec(memory_space=pltpu.VMEM)
    f32 = jnp.float32
    tile = (unit, lanes)
    piece = pltpu.VMEM((chans, TERMS, sub, cols), f32)
    operand = pltpu.VMEM((chans, TERMS * lanes, 2 * cols), jnp.bfloat16)
    columns = pltpu.VMEM((CHUNKS, slabs, TERMS) + tile, f32)
    wide = pltpu.VMEM((CHUNKS, chans, slabs) + tile, f32)
    others = pltpu.VMEM((CHUNKS, chans - 1, slabs) + tile, f32)
    sorted_tiles = pltpu.VMEM((CHUNKS, chans, unit, slabs * lanes), f32)
    return pl.pallas_call(
        functools.partial(middle_kernel, slabs, chans),
        out_shape=jax.ShapeDtypeStruct((TERMS, rows, cols), f32),
        in_specs=[vmem] * 10,
        out_specs=vmem,
        scratch_shapes=[
            pltpu.VMEM((cols // lanes, TERMS, rows, lanes), f32),
            piece, piece, operand, operand,
            pltpu.VMEM((chans, TERMS * lanes, 2 * cols), f32),
            piece, piece, columns, columns,
            columns, others, wide, others, wide, columns,
            pltpu.VMEM((chans, 8, lanes), f32),
            pltpu.VMEM((chans * slabs,) + tile, f32),
            sorted_tiles, sorted_tiles,
        ]
        + [pltpu.SemaphoreType.DMA((CHUNKS, slabs))] * 2
        + [pltpu.SemaphoreType.DMA((CHUNKS, chans))] * 4
        + [pltpu.SemaphoreType.DMA((CHUNKS, slabs))] * 2
        + [pltpu.SemaphoreType.DMA((chans,))] * 6,
        compiler_params=pltpu.CompilerParams(
            collective_id=0, has_side_effects=True, vmem_limit_bytes=63 * 1024 * 1024
        ),
    )(
        taylor_models, gridded_vis[0], uv_weight[0],
        jnp.broadcast_to(freq_ratio[0] - 1.0, (8, lanes)),
        jnp.broadcast_to(robust_scale[0], (8, lanes)),
        jnp.asarray(high), jnp.asarray(low), sort_table(slabs, sub),
        jnp.asarray(xtab), jnp.asarray(turn),
    )


def solution(mesh):
    placed = (
        P(None, "slab", "chan"),
        P("chan", None, "slab", None),
        P("chan", "slab", None),
        P("chan"),
        P("chan"),
    )
    return jax.shard_map(
        local, mesh=mesh, in_specs=placed, out_specs=P(None, "slab", "chan"), check_vma=False
    )
```

```python
import functools
import math

import jax
import jax.numpy as jnp
import numpy as np
from jax import lax
from jax.experimental import pallas as pl
from jax.experimental.pallas import tpu as pltpu
from jax.sharding import PartitionSpec as P

PIX = 2048
TERMS = 2


HIGHEST = lax.Precision.HIGH


def dft_table(points, direction):
    steps_all = jnp.arange(points, dtype=jnp.int32)
    product = steps_all[:, None] * steps_all[None, :] % points
    angles = product.astype(jnp.float32) * (2.0 * math.pi / points)
    return (jnp.cos(angles), direction * jnp.sin(angles))


def twiddle_table(outer_points, inner_points, direction):
    outer_steps = jnp.arange(outer_points, dtype=jnp.int32)
    inner_steps = jnp.arange(inner_points, dtype=jnp.int32)
    overall = outer_points * inner_points
    product = outer_steps[:, None] * inner_steps[None, :] % overall
    angles = product.astype(jnp.float32) * (2.0 * math.pi / overall)
    return (jnp.cos(angles), direction * jnp.sin(angles))


def complex_product(formula, left_real, left_imag, table_real, table_imag):
    out_real = jnp.einsum(formula, left_real, table_real, precision=HIGHEST) - jnp.einsum(
        formula, left_imag, table_imag, precision=HIGHEST
    )
    out_imag = jnp.einsum(formula, left_real, table_imag, precision=HIGHEST) + jnp.einsum(
        formula, left_imag, table_real, precision=HIGHEST
    )
    return (out_real, out_imag)


def rotate(left_real, left_imag, table_real, table_imag):
    return (
        left_real * table_real - left_imag * table_imag,
        left_real * table_imag + left_imag * table_real,
    )


def local_general(taylor_models, gridded_vis, uv_weight, freq_ratio, robust_scale):
    inner_count = 128
    outer_count = PIX // inner_count
    chans = lax.axis_size("chan")
    slabs = lax.axis_size("slab")
    rows = taylor_models.shape[1]
    cols = taylor_models.shape[2]
    sub = rows // chans
    col_count = PIX // slabs
    outer_cos, outer_sin = dft_table(outer_count, -1.0)
    inner_cos, inner_sin = dft_table(inner_count, -1.0)
    twist_cos, twist_sin = twiddle_table(outer_count, inner_count, -1.0)
    offsets = lax.all_gather(freq_ratio, "chan", axis=0, tiled=True) - 1.0

    pieces = taylor_models.reshape(TERMS, chans, sub, cols).transpose(1, 0, 2, 3)
    pieces = lax.all_to_all(pieces, "chan", split_axis=0, concat_axis=0, tiled=True)
    layered = pieces.transpose(1, 2, 0, 3).reshape(TERMS * sub, outer_count, inner_count)
    part_real = jnp.einsum("yba,jb->yja", layered, outer_cos, precision=HIGHEST)
    part_imag = jnp.einsum("yba,jb->yja", layered, outer_sin, precision=HIGHEST)
    turned_real, turned_imag = rotate(part_real, part_imag, twist_cos, twist_sin)
    spec_real, spec_imag = complex_product(
        "yja,ka->kjy", turned_real, turned_imag, inner_cos, inner_sin
    )
    outgoing = jnp.stack(
        [
            spec_real.reshape(slabs, col_count, TERMS * sub),
            spec_imag.reshape(slabs, col_count, TERMS * sub),
        ],
        axis=1,
    )
    arrived = lax.all_to_all(outgoing, "slab", split_axis=0, concat_axis=0, tiled=True)
    arrived = arrived.reshape(slabs, 2, col_count, TERMS, sub)
    arrived = arrived.transpose(3, 1, 2, 0, 4).reshape(TERMS, 2, col_count, slabs * sub)
    mixed = arrived[0][None] + offsets[:, None, None, None] * arrived[1][None]
    mixed = lax.all_to_all(mixed, "chan", split_axis=0, concat_axis=0, tiled=True)
    columns = mixed.reshape(chans, 2, col_count, slabs, sub).transpose(1, 2, 3, 0, 4)
    layered_cols = columns.reshape(2, col_count, outer_count, inner_count)
    part_real, part_imag = complex_product(
        "uba,jb->uja", layered_cols[0], layered_cols[1], outer_cos, outer_sin
    )
    turned_real, turned_imag = rotate(part_real, part_imag, twist_cos, twist_sin)
    freq_real, freq_imag = complex_product(
        "uja,ka->ujk", turned_real, turned_imag, inner_cos, inner_sin
    )
    freq_real = freq_real / PIX
    freq_imag = freq_imag / PIX
    weight = (
        uv_weight[0]
        .astype(jnp.float32)
        .reshape(col_count, inner_count, outer_count)
        .transpose(0, 2, 1)
    )
    visible = (
        gridded_vis[0]
        .astype(jnp.float32)
        .reshape(2, col_count, inner_count, outer_count)
        .transpose(0, 1, 3, 2)
    )
    delta_real = visible[0] - weight * freq_real
    delta_imag = visible[1] - weight * freq_imag
    robust = 1.0 / (1.0 + robust_scale[0] * (delta_real * delta_real + delta_imag * delta_imag))
    weighted_real = robust * delta_real
    weighted_imag = robust * delta_imag
    back_real, back_imag = complex_product(
        "ujk,ak->uja", weighted_real, weighted_imag, inner_cos, -inner_sin
    )
    back_real, back_imag = rotate(back_real, back_imag, twist_cos, -twist_sin)
    back_real, back_imag = complex_product(
        "uja,bj->uba", back_real, back_imag, outer_cos, -outer_sin
    )
    back = jnp.stack([back_real, back_imag]).reshape(2, col_count, slabs, chans, sub)
    back = back.transpose(3, 0, 1, 2, 4).reshape(chans, 2, col_count, slabs * sub)
    back = lax.all_to_all(back, "chan", split_axis=0, concat_axis=0, tiled=True)
    total = jnp.stack(
        [jnp.sum(back * offsets[:, None, None, None] ** t, axis=0) for t in range(TERMS)]
    )
    total = total.reshape(TERMS, 2, col_count, slabs, sub).transpose(3, 1, 2, 0, 4)
    total = total.reshape(slabs, 2, col_count, TERMS * sub)
    total = lax.all_to_all(total, "slab", split_axis=0, concat_axis=0, tiled=True)
    layered_rows = total.transpose(1, 0, 2, 3).reshape(2, inner_count, outer_count, TERMS * sub)
    last_real, last_imag = complex_product(
        "kjy,ak->ajy", layered_rows[0], layered_rows[1], inner_cos, -inner_sin
    )
    last_real, last_imag = rotate(
        last_real, last_imag, twist_cos.T[:, :, None], -twist_sin.T[:, :, None]
    )
    image_out = jnp.einsum("ajy,bj->yba", last_real, outer_cos, precision=HIGHEST) + jnp.einsum(
        "ajy,bj->yba", last_imag, outer_sin, precision=HIGHEST
    )
    image_out = image_out.reshape(TERMS, sub, chans, cols).transpose(2, 0, 1, 3) / PIX
    tiles = lax.all_to_all(image_out, "chan", split_axis=0, concat_axis=0, tiled=True)
    return tiles.transpose(1, 0, 2, 3).reshape(TERMS, rows, cols)


CHUNKS = 8
GROUP = 8
MESH = pl.DeviceIdType.MESH


def lane_tables(slabs, chans, sub):
    j = np.arange(chans)[:, None, None, None]
    v0 = np.arange(slabs)[None, :, None, None]
    r = np.arange(sub)[None, None, :, None]
    k = np.arange(sub)[None, None, None, :]
    phase = ((chans * r + j) * (v0 + slabs * k)) % PIX
    cos = np.cos(2.0 * np.pi * phase / PIX) / PIX
    sin = -np.sin(2.0 * np.pi * phase / PIX) / PIX
    top = np.concatenate([cos, sin], axis=3)
    low = np.concatenate([-sin, cos], axis=3)
    table = np.concatenate([top, low], axis=2).reshape(chans * slabs, 2 * sub, 2 * sub)
    table = table.astype(np.float32)
    high = table.astype(jnp.bfloat16)
    return high, (table - high.astype(np.float32)).astype(jnp.bfloat16)


def column_tables(slabs, chans, span):
    u1 = np.arange(span).reshape(slabs, CHUNKS, span // (slabs * CHUNKS))
    u1 = u1.transpose(1, 0, 2).reshape(span, 1)
    angle = 2.0 * np.pi * ((u1 * np.arange(span)[None, :]) % span) / span
    table = np.concatenate([np.cos(angle), np.sin(angle)], axis=1).astype(np.float32)
    high = table.astype(jnp.bfloat16)
    low = (table - high.astype(np.float32)).astype(jnp.bfloat16)
    turn = 2.0 * np.pi * np.arange(chans)[:, None] * np.arange(span)[None, :] / PIX
    turn = np.stack([np.cos(turn), np.sin(turn)], axis=1).reshape(2 * chans, span)
    parts = [x.reshape(CHUNKS, span // CHUNKS, 2 * span) for x in (high, low)]
    return np.stack(parts, axis=1).reshape(2 * span, 2 * span), turn.astype(np.float32)


def sort_table(slabs, sub):
    source = jnp.arange(slabs * sub, dtype=jnp.int32)
    target = (source % slabs) * sub + source // slabs
    return (target[:, None] == source[None, :]).astype(jnp.bfloat16)


def middle_kernel(
    slabs, chans, m_ref, vis_ref, wt_ref, off_ref, rs_ref, high_ref, low_ref, sort_ref,
    xtab_ref, turn_ref, out_ref,
    stage, xsend, xrecv, ohigh, olow, acc, rsend, rrecv, g_ref, q_ref, zin, mix, spec, back, landed, qsend, offs, work, vsort, wsort,
    z_send, z_recv, c_send, c_recv, b_send, b_recv, q_send, q_recv, o_send, o_recv,
    x_send, x_recv, r_send, r_recv,
):
    slab = lax.axis_index("slab")
    chan = lax.axis_index("chan")
    unit = g_ref.shape[3]
    lanes = g_ref.shape[4]
    half = lanes // 2
    span = slabs * half

    def slab_peer(d):
        return lax.rem(slab + d, slabs)

    def slab_from(d):
        return lax.rem(slab + slabs - d, slabs)

    def chan_peer(d):
        return lax.rem(chan + d, chans)

    def chan_from(d):
        return lax.rem(chan + chans - d, chans)

    def z_copy(c, d, owner):
        return pltpu.make_async_remote_copy(
            src_ref=g_ref.at[c, slab_peer(d)], dst_ref=zin.at[c, owner],
            send_sem=z_send.at[c, d], recv_sem=z_recv.at[c, d],
            device_id=(chan, slab_peer(d)), device_id_type=MESH)

    def c_copy(c, d, owner):
        return pltpu.make_async_remote_copy(
            src_ref=mix.at[c, d - 1], dst_ref=spec.at[c, owner],
            send_sem=c_send.at[c, d], recv_sem=c_recv.at[c, d],
            device_id=(chan_peer(d), slab), device_id_type=MESH)

    def b_copy(c, d, owner):
        return pltpu.make_async_remote_copy(
            src_ref=back.at[c, d - 1], dst_ref=landed.at[c, owner],
            send_sem=b_send.at[c, d], recv_sem=b_recv.at[c, d],
            device_id=(chan_peer(d), slab), device_id_type=MESH)

    def q_copy(c, d, owner):
        return pltpu.make_async_remote_copy(
            src_ref=qsend.at[c, slab_peer(d)], dst_ref=q_ref.at[c, owner],
            send_sem=q_send.at[c, d], recv_sem=q_recv.at[c, d],
            device_id=(chan, slab_peer(d)), device_id_type=MESH)

    def o_copy(d, owner):
        return pltpu.make_async_remote_copy(
            src_ref=off_ref, dst_ref=offs.at[owner],
            send_sem=o_send.at[d], recv_sem=o_recv.at[d],
            device_id=(chan_peer(d), slab), device_id_type=MESH)

    def x_copy(d, owner):
        return pltpu.make_async_remote_copy(
            src_ref=xsend.at[chan_peer(d)], dst_ref=xrecv.at[owner],
            send_sem=x_send.at[d], recv_sem=x_recv.at[d],
            device_id=(chan_peer(d), slab), device_id_type=MESH)

    def r_copy(d, owner):
        return pltpu.make_async_remote_copy(
            src_ref=rsend.at[chan_peer(d)], dst_ref=rrecv.at[owner],
            send_sem=r_send.at[d], recv_sem=r_recv.at[d],
            device_id=(chan_peer(d), slab), device_id_type=MESH)

    sub = half
    cols = m_ref.shape[2]
    quarter = unit // chans
    for m in range(TERMS):
        for q in range(cols // lanes):
            at = pl.ds(q * lanes, lanes)
            stage[q, m] = m_ref[m, :, at]
            for j in range(chans):
                xsend[j, m, :, at] = stage[q, m, pl.ds(j, sub, stride=chans), :]

    barrier = pltpu.get_barrier_semaphore()
    for d in range(1, slabs):
        pl.semaphore_signal(barrier, inc=1, device_id=(chan, slab_peer(d)), device_id_type=MESH)
    for d in range(1, chans):
        pl.semaphore_signal(barrier, inc=1, device_id=(chan_peer(d), slab), device_id_type=MESH)
    pl.semaphore_wait(barrier, slabs + chans - 2)

    for d in range(1, chans):
        x_copy(d, chan).start()
    for d in range(1, chans):
        o_copy(d, chan).start()

    offs[chan] = off_ref[...]
    xrecv[chan] = xsend[chan]
    acc[...] = jnp.zeros_like(acc)

    @pl.loop(0, chans)
    def _(jj):
        at = pl.ds(pl.multiple_of(jj * span, span), span)
        dot = functools.partial(jnp.dot, preferred_element_type=jnp.float32)
        real, imag = dot(vis_ref[0, :, at], sort_ref[...]), dot(vis_ref[1, :, at], sort_ref[...])
        scale = dot(wt_ref[:, at], sort_ref[...])
        lower = lax.broadcasted_iota(jnp.int32, (unit, lanes), 1) < half
        for c in range(CHUNKS):
            for p in range(slabs // 2):
                re, im, wt = [
                    x[c * unit : (c + 1) * unit, p * lanes : (p + 1) * lanes]
                    for x in (real, imag, scale)
                ]
                even, odd = pl.ds(2 * p * lanes, lanes), pl.ds((2 * p + 1) * lanes, lanes)
                turned = pltpu.roll(wt, half, 1)
                vsort[c, jj, :, even] = jnp.where(lower, re, pltpu.roll(im, half, 1))
                vsort[c, jj, :, odd] = jnp.where(lower, pltpu.roll(re, half, 1), im)
                wsort[c, jj, :, even] = jnp.where(lower, wt, turned)
                wsort[c, jj, :, odd] = jnp.where(lower, turned, wt)

    for d in range(1, chans):
        o_copy(d, chan_from(d)).wait_recv()

    for d in range(1, chans):
        x_copy(d, chan_from(d)).wait_recv()

    def halves(x):
        high = x.astype(jnp.bfloat16)
        return high, (x - high.astype(jnp.float32)).astype(jnp.bfloat16)

    for m in range(TERMS):
        @pl.loop(0, sub // 16)
        def _(i):
            start = pl.multiple_of(i * 16, 16)
            x = [xrecv[c, m, pl.ds(start, 16), :] for c in range(chans)]
            s0, s1, t0, t1 = x[0] + x[2], x[0] - x[2], x[1] + x[3], x[1] - x[3]
            for u0 in range(chans):
                cos, sin = turn_ref[2 * u0 : 2 * u0 + 1, :], turn_ref[2 * u0 + 1 : 2 * u0 + 2, :]
                if u0 % 2 == 0:
                    zr = s0 + t0 if u0 == 0 else s0 - t0
                    real, imag = zr * cos, -(zr * sin)
                else:
                    zi = -t1 if u0 == 1 else t1
                    real, imag = s1 * cos + zi * sin, zi * cos - s1 * sin
                one = pl.ds(pl.multiple_of(m * lanes + i * 16, 16), 16)
                two = pl.ds(pl.multiple_of(m * lanes + half + i * 16, 16), 16)
                left, right = pl.ds(0, cols), pl.ds(cols, cols)
                rh, rl = halves(real)
                ih, il = halves(imag)
                for into, re, im in ((ohigh, rh, ih), (olow, rl, il)):
                    into[u0, one, left] = re
                    into[u0, one, right] = im
                    into[u0, two, left] = im
                    into[u0, two, right] = -re

    @pl.loop(0, CHUNKS)
    def _(c):
        count = slabs * quarter
        at = pl.multiple_of(c * 2 * count, 2 * count)
        both, wide = xtab_ref[pl.ds(at, 2 * count), :], xtab_ref[pl.ds(at, count), :]
        dot = functools.partial(
            lax.dot_general, dimension_numbers=(((1,), (1,)), ((), ())),
            preferred_element_type=jnp.float32)
        for u0 in range(chans):
            found = dot(both, ohigh[u0])
            found = found[:count] + (found[count:] + dot(wide, olow[u0]))
            for s in range(slabs):
                for m in range(TERMS):
                    g_ref[c, s, m, pl.ds(u0, quarter, stride=chans), :] = found[
                        s * quarter : (s + 1) * quarter, m * lanes : (m + 1) * lanes
                    ]
        for d in range(1, slabs):
            z_copy(c, d, slab).start()
        zin[c, slab] = g_ref[c, slab]

    lane = lax.broadcasted_iota(jnp.int32, (GROUP, lanes), 1)
    sign = jnp.where(lane < half, -1.0, 1.0)

    def times_i(x, direction):
        return pltpu.roll(x, half, 1) * (sign * direction)

    def four(x0, x1, x2, x3, direction):
        s0, s1, t0, t1 = x0 + x2, x0 - x2, x1 + x3, times_i(x1 - x3, direction)
        return s0 + t0, s1 + t1, s0 - t0, s1 - t1

    def eight(x, direction):
        root = math.sqrt(0.5)
        even = four(x[0], x[2], x[4], x[6], direction)
        odd = four(x[1], x[3], x[5], x[7], direction)
        odd = (
            odd[0],
            (odd[1] + times_i(odd[1], direction)) * root,
            times_i(odd[2], direction),
            (times_i(odd[3], direction) - odd[3]) * root,
        )
        return [e + o for e, o in zip(even, odd)] + [e - o for e, o in zip(even, odd)]

    def split(x):
        high = x.astype(jnp.bfloat16)
        return high, (x - high.astype(jnp.float32)).astype(jnp.bfloat16)

    def product(x, t, dims):
        high, low = split(x)
        dot = functools.partial(
            lax.dot_general, dimension_numbers=(dims, ((), ())),
            preferred_element_type=jnp.float32)
        both = dot(jnp.concatenate([high, low], axis=0), high_ref[t])
        return both[:unit] + (both[unit:] + dot(high, low_ref[t]))

    def spread(c):
        for d in range(1, slabs):
            z_copy(c, d, slab_from(d)).wait_recv()

        @pl.loop(0, slabs)
        def _(s):
            base, slope = zin[c, s, 0], zin[c, s, 1]
            spec[c, chan, s] = base + offs[chan][0:1, :] * slope
            for d in range(1, chans):
                mix[c, d - 1, s] = base + offs[chan_peer(d)][0:1, :] * slope

        for d in range(1, chans):
            c_copy(c, d, chan).start()

    def weigh(c):
        for d in range(1, chans):
            c_copy(c, d, chan_from(d)).wait_recv()
        damping = rs_ref[0:1, :]

        @pl.loop(0, unit // GROUP)
        def _(i):
            rows = pl.ds(pl.multiple_of(i * GROUP, GROUP), GROUP)
            for j in range(chans):
                out = eight([spec[c, j, s, rows, :] for s in range(slabs)], -1.0)
                for v0 in range(slabs):
                    work[j * slabs + v0, rows, :] = out[v0]

        @pl.loop(0, chans)
        def _(j):
            tiles = [j * slabs + v0 for v0 in range(slabs)]
            done = [product(work[t], t, ((1,), (0,))) for t in tiles]
            for t, x in zip(tiles, done):
                work[t] = x

        @pl.loop(0, unit // GROUP)
        def _(i):
            rows = pl.ds(pl.multiple_of(i * GROUP, GROUP), GROUP)
            for v0 in range(slabs):
                at = pl.ds(v0 * lanes, lanes)
                found = four(*[work[j * slabs + v0, rows, :] for j in range(chans)], -1.0)
                kept = []
                for jj in range(chans):
                    delta = vsort[c, jj, rows, at] - wsort[c, jj, rows, at] * found[jj]
                    power = delta * delta
                    power = power + pltpu.roll(power, half, 1)
                    kept.append(delta / (1.0 + damping * power))
                out = four(*kept, 1.0)
                for j in range(chans):
                    work[j * slabs + v0, rows, :] = out[j]

        @pl.loop(0, chans)
        def _(j):
            tiles = [j * slabs + v0 for v0 in range(slabs)]
            done = [product(work[t], t, ((1,), (1,))) for t in tiles]
            for t, x in zip(tiles, done):
                work[t] = x

        @pl.loop(0, unit // GROUP)
        def _(i):
            rows = pl.ds(pl.multiple_of(i * GROUP, GROUP), GROUP)
            for d in range(chans):
                first = chan_peer(d) * slabs
                out = eight([work[first + v0, rows, :] for v0 in range(slabs)], 1.0)
                for s in range(slabs):
                    if d == 0:
                        landed[c, chan, s, rows, :] = out[s]
                    else:
                        back[c, d - 1, s, rows, :] = out[s]

        for d in range(1, chans):
            b_copy(c, d, chan).start()

    def gather(c):
        for d in range(1, chans):
            b_copy(c, d, chan_from(d)).wait_recv()

        @pl.loop(0, slabs)
        def _(s):
            parts = [landed[c, j, s] for j in range(chans)]
            qsend[c, s, 0] = (parts[0] + parts[1]) + (parts[2] + parts[3])
            scaled = [parts[j] * offs[j][0:1, :] for j in range(chans)]
            qsend[c, s, 1] = (scaled[0] + scaled[1]) + (scaled[2] + scaled[3])

        q_ref[c, slab] = qsend[c, slab]
        for d in range(1, slabs):
            q_copy(c, d, slab).start()

    def finish(c):
        for d in range(1, slabs):
            q_copy(c, d, slab_from(d)).wait_recv()
        count = slabs * quarter
        at = pl.multiple_of(c * 2 * count, 2 * count)
        th, tl = xtab_ref[pl.ds(at, count), :], xtab_ref[pl.ds(at + count, count), :]
        dot = functools.partial(jnp.dot, preferred_element_type=jnp.float32)
        for u0 in range(chans):
            held = jnp.concatenate(
                [
                    jnp.concatenate(
                        [
                            q_ref[c, s, t, pl.ds(u0, quarter, stride=chans), :]
                            for t in range(TERMS)
                        ],
                        axis=1,
                    )
                    for s in range(slabs)
                ],
                axis=0,
            )
            qh, ql = halves(held.T)
            found = dot(jnp.concatenate([qh, ql], axis=0), th)
            acc[u0] += found[: TERMS * lanes] + (found[TERMS * lanes :] + dot(qh, tl))

    @pl.loop(0, CHUNKS + 4)
    def _(step):
        @pl.when(step < CHUNKS)
        def _():
            spread(step)

        @pl.when(jnp.logical_and(step >= 1, step < CHUNKS + 1))
        def _():
            weigh(step - 1)

        @pl.when(jnp.logical_and(step >= 3, step < CHUNKS + 3))
        def _():
            gather(step - 3)

        @pl.when(step >= 4)
        def _():
            finish(step - 4)

    for t in range(TERMS):
        @pl.loop(0, sub // GROUP)
        def _(i):
            rows = pl.ds(pl.multiple_of(i * GROUP, GROUP), GROUP)
            one = pl.ds(pl.multiple_of(t * lanes + i * GROUP, GROUP), GROUP)
            two = pl.ds(pl.multiple_of(t * lanes + half + i * GROUP, GROUP), GROUP)
            left, right = pl.ds(0, cols), pl.ds(cols, cols)
            real, imag = [], []
            for u0 in range(chans):
                cos, sin = turn_ref[2 * u0 : 2 * u0 + 1, :], turn_ref[2 * u0 + 1 : 2 * u0 + 2, :]
                yr = acc[u0, one, left] - acc[u0, two, right]
                yi = acc[u0, one, right] + acc[u0, two, left]
                real.append(yr * cos - yi * sin)
                imag.append(yr * sin + yi * cos)
            e0, e1 = real[0] + real[2], real[0] - real[2]
            o0, o1 = real[1] + real[3], imag[3] - imag[1]
            rsend[0, t, rows, :] = e0 + o0
            rsend[1, t, rows, :] = e1 + o1
            rsend[2, t, rows, :] = e0 - o0
            rsend[3, t, rows, :] = e1 - o1

    for d in range(1, chans):
        r_copy(d, chan).start()
    rrecv[chan] = rsend[chan]
    for d in range(1, chans):
        r_copy(d, chan_from(d)).wait_recv()
    for t in range(TERMS):
        for q in range(cols // lanes):
            at = pl.ds(q * lanes, lanes)
            for j in range(chans):
                stage[q, t, pl.ds(j, sub, stride=chans), :] = rrecv[j, t, :, at]
            out_ref[t, :, at] = stage[q, t]

    @pl.loop(0, CHUNKS)
    def _(c):
        for d in range(1, slabs):
            q_copy(c, d, slab).wait_send()
            z_copy(c, d, slab).wait_send()
        for d in range(1, chans):
            c_copy(c, d, chan).wait_send()
            b_copy(c, d, chan).wait_send()

    for d in range(1, chans):
        o_copy(d, chan).wait_send()
        x_copy(d, chan).wait_send()
        r_copy(d, chan).wait_send()


def local(taylor_models, gridded_vis, uv_weight, freq_ratio, robust_scale):
    chans = lax.axis_size("chan")
    slabs = lax.axis_size("slab")
    rows = taylor_models.shape[1]
    cols = taylor_models.shape[2]
    sub = rows // chans
    if slabs != 8 or chans != 4 or 2 * sub != 128:
        return local_general(taylor_models, gridded_vis, uv_weight, freq_ratio, robust_scale)
    unit = PIX // slabs // CHUNKS
    lanes = 2 * sub
    high, low = lane_tables(slabs, chans, sub)
    xtab, turn = column_tables(slabs, chans, cols)
    vmem = pl.BlockSpec(memory_space=pltpu.VMEM)
    f32 = jnp.float32
    tile = (unit, lanes)
    piece = pltpu.VMEM((chans, TERMS, sub, cols), f32)
    operand = pltpu.VMEM((chans, TERMS * lanes, 2 * cols), jnp.bfloat16)
    columns = pltpu.VMEM((CHUNKS, slabs, TERMS) + tile, f32)
    wide = pltpu.VMEM((CHUNKS, chans, slabs) + tile, f32)
    others = pltpu.VMEM((CHUNKS, chans - 1, slabs) + tile, f32)
    sorted_tiles = pltpu.VMEM((CHUNKS, chans, unit, slabs * lanes), f32)
    return pl.pallas_call(
        functools.partial(middle_kernel, slabs, chans),
        out_shape=jax.ShapeDtypeStruct((TERMS, rows, cols), f32),
        in_specs=[vmem] * 10,
        out_specs=vmem,
        scratch_shapes=[
            pltpu.VMEM((cols // lanes, TERMS, rows, lanes), f32),
            piece, piece, operand, operand,
            pltpu.VMEM((chans, TERMS * lanes, 2 * cols), f32),
            piece, piece, columns, columns,
            columns, others, wide, others, wide, columns,
            pltpu.VMEM((chans, 8, lanes), f32),
            pltpu.VMEM((chans * slabs,) + tile, f32),
            sorted_tiles, sorted_tiles,
        ]
        + [pltpu.SemaphoreType.DMA((CHUNKS, slabs))] * 2
        + [pltpu.SemaphoreType.DMA((CHUNKS, chans))] * 4
        + [pltpu.SemaphoreType.DMA((CHUNKS, slabs))] * 2
        + [pltpu.SemaphoreType.DMA((chans,))] * 6,
        compiler_params=pltpu.CompilerParams(
            collective_id=0, has_side_effects=True, vmem_limit_bytes=63 * 1024 * 1024
        ),
    )(
        taylor_models, gridded_vis[0], uv_weight[0],
        jnp.broadcast_to(freq_ratio[0] - 1.0, (8, lanes)),
        jnp.broadcast_to(robust_scale[0], (8, lanes)),
        jnp.asarray(high), jnp.asarray(low), sort_table(slabs, sub),
        jnp.asarray(xtab), jnp.asarray(turn),
    )


def solution(mesh):
    placed = (
        P(None, "slab", "chan"),
        P("chan", None, "slab", None),
        P("chan", "slab", None),
        P("chan"),
        P("chan"),
    )
    return jax.shard_map(
        local, mesh=mesh, in_specs=placed, out_specs=P(None, "slab", "chan"), check_vma=False
    )
```
